128 devices in a mesh: gy: 8 (over z, y_hi), gx: 16 (over y_lo, x, core).
Axes of the slice: x: 4, y: 4 (y_hi: 2, y_lo: 2; y = y_hi * 2 + y_lo), z: 4, core: 2. Of those that a mesh axis runs over, the one named last changes fastest.
Arguments:
- coefficients: float32 [9, 256, 512], P(None, 'gy', 'gx'), may hold values from -2.1 to 2.1
- vectors: float32 [256, 512, 2048], P('gy', 'gx'), may hold values from -6 to 6
Outputs:
- normal: float32 [25, 256, 512], P(None, 'gy', 'gx')
- image: float32 [256, 512, 2048], P('gy', 'gx')
The draws below stay inside these ranges and needn't reach their ends.
All inputs are finite; a program needn't handle non-finite values.
Results may differ from the reference program's by a relative error of at most 0.00002.
Values sent between devices are 32-bit elements; how exact they have to be, the bound alone decides.
A program may use at most 192 MiB of HBM per device.

```python
import math
import jax
import jax.numpy as jnp
from jax import lax

NV = 2048
NX = 256
NY = 512


def block_levels(rng, shape, shards, least, largest):
    def one(axis_at, parts):
        heights = jax.random.uniform(jax.random.fold_in(jax.random.fold_in(rng, 6), axis_at), (parts,), jnp.float32, least / len(shards), largest / len(shards))
        return jnp.repeat(jnp.exp(heights), shape[axis_at] // parts).reshape((-1,) + (1,) * (len(shape) - axis_at - 1))

    loudness = one(*shards[0])
    for cut in shards[1:]:
        loudness = loudness * one(*cut)
    return loudness


def centred(stream_key, shape, spread, limit, cuts=(), held_as=jnp.bfloat16):
    gain = block_levels(stream_key, shape, cuts, -0.22, 0.18) if cuts else 1.0
    drawn = jax.random.normal(stream_key, shape, jnp.float32) * spread * gain
    return jnp.minimum(jnp.maximum(drawn, -limit), limit).astype(held_as)


def setup_inputs(seed: int = 0) -> dict:
    keys = jax.random.split(jax.random.key(seed), 3)
    coefficients = centred(keys[0], (9, NX, NY), 0.35, 2.1, ((1, 8), (2, 16)), jnp.float32)
    vectors = centred(keys[1], (NX, NY, NV), 1.0, 6.0, ((0, 8), (1, 16)), jnp.float32)
    return dict(coefficients=coefficients, vectors=vectors)


def reference(coefficients, vectors):
    row_pos = jnp.arange(NX, dtype=jnp.int32)[:, None]
    col_pos = jnp.arange(NY, dtype=jnp.int32)[None, :]
    pieces = []
    for k in range(9):
        a = k // 3 - 1
        b = k % 3 - 1
        inside = (row_pos + a >= 0) & (row_pos + a < NX) & (col_pos + b >= 0) & (col_pos + b < NY)
        pieces.append(jnp.where(inside, coefficients[k], jnp.zeros_like(coefficients[k])))
    masked = jnp.stack(pieces)
    padded = jnp.pad(masked, ((0, 0), (1, 1), (1, 1)))
    terms = [jnp.zeros((NX, NY), coefficients.dtype) for slot in range(25)]
    for k in range(9):
        a = k // 3 - 1
        b = k % 3 - 1
        for m in range(9):
            e = (m // 3) - (k // 3)
            f = (m % 3) - (k % 3)
            slot_index = (e + 2) * 5 + (f + 2)
            first = padded[k, 1 - a:1 - a + NX, 1 - b:1 - b + NY]
            second = padded[m, 1 - a:1 - a + NX, 1 - b:1 - b + NY]
            terms[slot_index] = terms[slot_index] + first * second
    normal = jnp.stack(terms)
    block = math.gcd(NV, 128)

    def one_block(step, image):
        part = lax.dynamic_slice_in_dim(vectors, step * block, block, 2)
        wide = jnp.pad(part, ((2, 2), (2, 2), (0, 0)))
        total = jnp.zeros((NX, NY, block), vectors.dtype)
        for e in range(-2, 3):
            for f in range(-2, 3):
                slot_index = (e + 2) * 5 + (f + 2)
                total = total + normal[slot_index][:, :, None] * wide[2 + e:2 + e + NX, 2 + f:2 + f + NY, :]
        return lax.dynamic_update_slice_in_dim(image, total, step * block, 2)

    image = lax.fori_loop(0, NV // block, one_block, jnp.zeros_like(vectors))
    return normal, image
```

```python
import functools

import jax
import jax.numpy as jnp
from jax import lax
from jax.experimental import pallas as pl
from jax.experimental.pallas import tpu as pltpu
from jax.sharding import PartitionSpec as P

MESH = pl.DeviceIdType.MESH
F32 = jnp.float32
BF16 = jnp.bfloat16
STEPS = ((-1, 0), (1, 0), (0, -1), (0, 1), (-1, -1), (-1, 1), (1, -1), (1, 1))
UP, DOWN, LEFT, RIGHT = 0, 1, 2, 3
CHUNKS = 8
SLOTS = [((m // 3 - k // 3) + 2) * 5 + (m % 3 - k % 3) + 2 for k in range(9) for m in range(9)]


def kernel(
    rows_total, cols_total,
    coef_hbm, v_hbm, normal_ref, image_ref,
    coef, padded, flipped, shifted, nts,
    v_vm, up_vm, down_vm, col_vm, col_out, corner_out,
    row_msg, col_msg, heard,
    t_hi, t_lo, w_hi, w_lo,
    load_sem, coef_sem, msg_send, msg_recv, row_send, row_recv, col_send, col_recv, cor_send, cor_recv,
):
    gy = lax.axis_index("gy")
    gx = lax.axis_index("gx")
    ny = lax.axis_size("gy")
    nx = lax.axis_size("gx")
    rows, cols, nv = v_hbm.shape
    width = nv // CHUNKS

    def exists(n):
        dy, dx = STEPS[n]
        return (gy + dy >= 0) & (gy + dy < ny) & (gx + dx >= 0) & (gx + dx < nx)

    def at(n):
        dy, dx = STEPS[n]
        return (gy + dy, gx + dx)

    def lanes(i):
        return pl.ds(pl.multiple_of(i * width, width), width)

    def load(i):
        return pltpu.make_async_copy(v_hbm.at[:, :, lanes(i)], v_vm.at[:, :, lanes(i)], load_sem.at[i])

    def row_copy(s, i):
        src = v_hbm.at[0:2, :, lanes(i)] if s == UP else v_hbm.at[rows - 2:rows, :, lanes(i)]
        dst = down_vm if s == UP else up_vm
        return pltpu.make_async_remote_copy(
            src_ref=src, dst_ref=dst.at[:, :, lanes(i)], send_sem=row_send.at[s, i],
            recv_sem=row_recv.at[s, i], device_id=at(s), device_id_type=MESH)

    def col_copy(s, i):
        j = 2 - 2 * s
        return pltpu.make_async_remote_copy(
            src_ref=col_out.at[s, :, :, lanes(i)], dst_ref=col_vm.at[j:j + 2, 0:rows, lanes(i)],
            send_sem=col_send.at[s, i], recv_sem=col_recv.at[s, i], device_id=at(LEFT + s), device_id_type=MESH)

    def cor_copy(s, i):
        j = 2 - 2 * s
        return pltpu.make_async_remote_copy(
            src_ref=corner_out.at[s, :, :, lanes(i)], dst_ref=col_vm.at[j:j + 2, rows:rows + 8, lanes(i)],
            send_sem=cor_send.at[s, i], recv_sem=cor_recv.at[s, i], device_id=at(LEFT + s), device_id_type=MESH)

    def msg_copy(n):
        dy, dx = STEPS[n]
        src = row_msg.at[(dy + 1) // 2] if dy else col_msg.at[(dx + 1) // 2]
        return pltpu.make_async_remote_copy(
            src_ref=src, dst_ref=heard.at[n], send_sem=msg_send.at[n], recv_sem=msg_recv.at[n],
            device_id=at(n), device_id_type=MESH)

    opposite = [STEPS.index((-dy, -dx)) for dy, dx in STEPS]

    def when(pred, f):
        pl.when(pred)(f)

    take_coef = pltpu.make_async_copy(coef_hbm, coef, coef_sem)
    take_coef.start()
    for i in range(CHUNKS):
        load(i).start()

    barrier = pltpu.get_barrier_semaphore()
    known = jnp.int32(0)
    for n in range(8):
        when(exists(n), lambda n=n: pl.semaphore_signal(barrier, inc=1, device_id=at(n), device_id_type=MESH))
        known = known + exists(n).astype(jnp.int32)
    pl.semaphore_wait(barrier, known)

    def send_rows(i):
        for s in (UP, DOWN):
            when(exists(s), lambda s=s: row_copy(s, i).start())

    send_rows(0)
    padded[...] = jnp.zeros_like(padded)
    row_msg[...] = jnp.zeros_like(row_msg)
    col_msg[...] = jnp.zeros_like(col_msg)
    flipped[...] = jnp.zeros_like(flipped)
    take_coef.wait()
    padded[0:9, :, 0:cols] = coef[...]
    lane = lax.broadcasted_iota(jnp.int32, (8, 128), 1)
    for e, r in ((0, 0), (1, rows - 1)):
        for k in range(8):
            row_msg[e, k:k + 1, :] = padded[k, r:r + 1, :]
        last = pltpu.roll(jnp.broadcast_to(padded[8, r:r + 1, :], (8, 128)), 32, 1)
        row_msg[e] = jnp.where((lane >= 32) & (lane < 64), last, row_msg[e])
    for g in range(3):
        turned = padded[4 * g:4 * g + 4].reshape(128, 128).T
        col_msg[0, g:g + 1, :] = turned[0:1]
        col_msg[1, g:g + 1, :] = turned[cols - 1:cols]
        flipped[g, 1:cols + 1, :] = turned[0:cols]
    for n in range(8):
        when(exists(n), lambda n=n: msg_copy(n).start())

    def rest(i, c):
        send_rows(i)
        return c

    lax.fori_loop(1, CHUNKS, rest, 0)

    corner_out[...] = jnp.zeros_like(corner_out)

    def clear(ref):
        ref[...] = jnp.zeros_like(ref)

    when(jnp.logical_not(exists(UP)), lambda: clear(up_vm))
    when(jnp.logical_not(exists(DOWN)), lambda: clear(down_vm))
    when(jnp.logical_not(exists(LEFT)), lambda: clear(col_vm.at[0:2]))
    when(jnp.logical_not(exists(RIGHT)), lambda: clear(col_vm.at[2:4]))

    def pack(i, c):
        load(i).wait()
        for s in (0, 1):
            for j in (0, 1):
                col = j if s == 0 else cols - 2 + j
                for r in range(0, rows, 8):
                    col_out[s, j, r:r + 8, lanes(i)] = v_vm[r:r + 8, col, lanes(i)]
        for s in (0, 1):
            when(exists(LEFT + s), lambda s=s: col_copy(s, i).start())
        return c

    lax.fori_loop(0, CHUNKS, pack, 0)

    for n in range(8):
        when(exists(opposite[n]), lambda n=n: msg_copy(n).wait_recv())

    def from_side(n):
        return heard[opposite[n]]

    for g in range(3):
        flipped[g, 0:1, :] = jnp.where(exists(LEFT), from_side(LEFT)[g:g + 1], 0.0)
        flipped[g, cols + 1:cols + 2, :] = jnp.where(exists(RIGHT), from_side(RIGHT)[g:g + 1], 0.0)

    def rim(side, left, right):
        out = []
        for own, a, b in ((1, 97, 33), (97, 65, 1)):
            x = jnp.where(exists(side), pltpu.roll(from_side(side), own, 1), 0.0)
            x = jnp.where((lane == 0), jnp.where(exists(left), pltpu.roll(from_side(left), a, 1), 0.0), x)
            x = jnp.where((lane == cols + 1), jnp.where(exists(right), pltpu.roll(from_side(right), b, 1), 0.0), x)
            out.append(x)
        return out

    above = rim(UP, 4, 5)
    below = rim(DOWN, 6, 7)
    er = lax.broadcasted_iota(jnp.int32, (40, 128), 0)
    ec = lax.broadcasted_iota(jnp.int32, (40, 128), 1)
    row_at = gy * rows + er - 1
    col_at = gx * cols + ec - 1
    inside = (er < rows + 2) & (ec < cols + 2) & (row_at >= 0) & (row_at < rows_total) & (col_at >= 0) & (col_at < cols_total)
    for g in range(3):
        back = flipped[g].T
        for h in range(4):
            k = 4 * g + h
            if k < 9:
                a, b = k // 3 - 1, k % 3 - 1
                shifted[0, k, 1:rows + 1, :] = back[32 * h:32 * h + rows]
                which, line = (0, k) if k < 8 else (1, 0)
                shifted[0, k, 0:1, :] = above[which][line:line + 1]
                shifted[0, k, rows + 1:rows + 2, :] = below[which][line:line + 1]
                keep = inside & (row_at + a >= 0) & (row_at + a < rows_total) & (col_at + b >= 0) & (col_at + b < cols_total)
                x = jnp.where(keep, shifted[0, k], 0.0)
                shifted[0, k] = x
                shifted[1, k] = pltpu.roll(x, 127, 1)
                shifted[2, k] = pltpu.roll(x, 126, 1)
    terms = []
    for slot in range(25):
        total = None
        for at_pair in range(81):
            if SLOTS[at_pair] == slot:
                k, m = at_pair // 9, at_pair % 9
                a, b = k // 3 - 1, k % 3 - 1
                term = shifted[1 - b, k, 1 - a:1 - a + rows, :] * shifted[1 - b, m, 1 - a:1 - a + rows, :]
                total = term if total is None else total + term
        normal_ref[slot] = total[:, 0:cols]
        terms.append(total)
    for g in range(7):
        group = terms[4 * g:4 * g + 4]
        while len(group) < 4:
            group.append(jnp.zeros_like(group[0]))
        turned = jnp.concatenate(group, axis=0).T[0:cols]
        nts[0, g] = turned
        for b in range(1, 4):
            nts[b, g] = pltpu.roll(turned, 128 - 8 * b, 1)

    lane32 = lax.broadcasted_iota(jnp.int32, (cols, 128), 1)
    cell = lax.broadcasted_iota(jnp.int32, (cols, 128), 0)
    own_at, side_at = {}, {}
    for f in range(-2, 3):
        t = cell + f
        own_at[f] = jnp.where((t >= 0) & (t < cols), t, -1000)
        side_at[f] = jnp.where(t == -2, 0, jnp.where(t == -1, 32, jnp.where(t == cols, 64, jnp.where(t == cols + 1, 96, -1000))))

    def build(b, c):
        for rl in range(8):
            own = [jnp.zeros((cols, 128), F32) for _ in range(3)]
            side = jnp.zeros((cols, 128), F32)
            for e in range(-2, 3):
                spot = rl + e + 2
                tile, q = spot // 4, spot % 4
                row = b * 8 + rl + e
                slot = jnp.where(row < 0, 18 + row, row)
                slot = jnp.where(b == 3, jnp.where(row < rows, row - 16, row - 14), slot)
                for f in range(-2, 3):
                    index = (e + 2) * 5 + f + 2
                    at_lane = (index % 4) * 32 + rl
                    column = jnp.broadcast_to(nts[b, index // 4][:, at_lane:at_lane + 1], (cols, 128))
                    own[tile] = jnp.where(lane32 - 32 * q == own_at[f], column, own[tile])
                    if f:
                        side = jnp.where(lane32 - slot == side_at[f], column, side)
            for tile, x in enumerate(own + [side]):
                hi = x.astype(BF16)
                t_hi[b, rl * 32:rl * 32 + 32, tile * 128:tile * 128 + 128] = hi
                t_lo[b, rl * 32:rl * 32 + 32, tile * 128:tile * 128 + 128] = (x - hi.astype(F32)).astype(BF16)
        return c

    lax.fori_loop(0, 4, build, 0)

    def halves(x):
        hi = x.astype(BF16)
        return hi, (x - hi.astype(F32)).astype(BF16)

    def put(block, start, hi, lo):
        w_hi[block, start:start + hi.shape[0], :] = hi
        w_lo[block, start:start + hi.shape[0], :] = lo

    def compute(i):
        at_i = lanes(i)
        for s in (0, 1):
            when(exists(LEFT + 1 - s), lambda s=s: (col_copy(s, i).wait_recv(), cor_copy(s, i).wait_recv())[0])
        for q in range(4):
            hi, lo = halves(v_vm[8 * q:8 * q + 8, :, at_i].reshape(256, width))
            put(q, 64, hi, lo)
            if q > 0:
                put(q - 1, 320, hi[0:64], lo[0:64])
            if q < 3:
                put(q + 1, 0, hi[192:256], lo[192:256])
        put(0, 0, *halves(up_vm[:, :, at_i].reshape(64, width)))
        put(3, 320, *halves(down_vm[:, :, at_i].reshape(64, width)))
        for j in range(4):
            hi, lo = halves(col_vm[j, 0:32, at_i])
            chi, clo = halves(jnp.concatenate([col_vm[j, 32:40, at_i], jnp.zeros((8, width), F32)], axis=0))
            put(0, 384 + 32 * j, hi[0:16], lo[0:16])
            put(0, 400 + 32 * j, chi, clo)
            put(1, 384 + 32 * j, hi, lo)
            put(2, 384 + 32 * j, hi, lo)
            put(3, 384 + 32 * j, hi[16:32], lo[16:32])
            put(3, 400 + 32 * j, chi, clo)
        for q in range(4):
            y = jnp.dot(t_hi[q], w_hi[q], preferred_element_type=F32)
            y = y + jnp.dot(t_lo[q], w_hi[q], preferred_element_type=F32)
            y = y + jnp.dot(t_hi[q], w_lo[q], preferred_element_type=F32)
            image_ref[8 * q:8 * q + 8, :, at_i] = y.reshape(8, cols, width)

    def main(i, c):
        for s in (UP, DOWN):
            when(exists(1 - s), lambda s=s: row_copy(s, i).wait_recv())
        for s in (0, 1):
            for j in (0, 1):
                col = j if s == 0 else cols - 2 + j
                for h in (0, 1):
                    corner_out[s, j, h:h + 1, lanes(i)] = up_vm[h, col:col + 1, lanes(i)]
                    corner_out[s, j, 2 + h:3 + h, lanes(i)] = down_vm[h, col:col + 1, lanes(i)]
            when(exists(LEFT + s), lambda s=s: cor_copy(s, i).start())
        when(i > 0, lambda: compute(i - 1))
        return c

    lax.fori_loop(0, CHUNKS, main, 0)
    compute(CHUNKS - 1)

    def finish(i, c):
        for s in (0, 1):
            when(exists(s), lambda s=s: row_copy(s, i).wait_send())
            when(exists(LEFT + s), lambda s=s: (col_copy(s, i).wait_send(), cor_copy(s, i).wait_send())[0])
        return c

    lax.fori_loop(0, CHUNKS, finish, 0)
    for n in range(8):
        when(exists(n), lambda n=n: msg_copy(n).wait_send())


def per_device(rows_total, cols_total, coefficients, vectors):
    _, rows, cols = coefficients.shape
    nv = vectors.shape[2]
    width = nv // CHUNKS
    dma = pltpu.SemaphoreType.DMA
    return pl.pallas_call(
        functools.partial(kernel, rows_total, cols_total),
        out_shape=(pltpu.VMEM((25, rows, cols), F32), pltpu.VMEM((rows, cols, nv), F32)),
        in_specs=[pl.BlockSpec(memory_space=pltpu.HBM)] * 2,
        out_specs=(pl.BlockSpec(memory_space=pltpu.VMEM),) * 2,
        scratch_shapes=[
            pltpu.VMEM((9, rows, cols), F32),
            pltpu.VMEM((12, rows, 128), F32),
            pltpu.VMEM((3, 128, 128), F32),
            pltpu.VMEM((3, 9, 40, 128), F32),
            pltpu.VMEM((4, 7, cols, 128), F32),
            pltpu.VMEM((rows, cols, nv), F32),
            pltpu.VMEM((2, cols, nv), F32),
            pltpu.VMEM((2, cols, nv), F32),
            pltpu.VMEM((4, rows + 8, nv), F32),
            pltpu.VMEM((2, 2, rows, nv), F32),
            pltpu.VMEM((2, 2, 8, nv), F32),
            pltpu.VMEM((2, 8, 128), F32),
            pltpu.VMEM((2, 8, 128), F32),
            pltpu.VMEM((8, 8, 128), F32),
            pltpu.VMEM((4, 256, 512), BF16),
            pltpu.VMEM((4, 256, 512), BF16),
            pltpu.VMEM((4, 512, width), BF16),
            pltpu.VMEM((4, 512, width), BF16),
            dma((CHUNKS,)), dma,
            dma((8,)), dma((8,)),
            dma((2, CHUNKS)), dma((2, CHUNKS)),
            dma((2, CHUNKS)), dma((2, CHUNKS)),
            dma((2, CHUNKS)), dma((2, CHUNKS)),
        ],
        compiler_params=pltpu.CompilerParams(collective_id=0, has_side_effects=True, vmem_limit_bytes=44 * 2**20),
    )(coefficients, vectors)


def solution(mesh):
    in_specs = (P(None, "gy", "gx"), P("gy", "gx", None))
    out_specs = (P(None, "gy", "gx"), P("gy", "gx", None))

    def whole(coefficients, vectors):
        body = functools.partial(per_device, coefficients.shape[1], coefficients.shape[2])
        return jax.shard_map(body, mesh=mesh, in_specs=in_specs, out_specs=out_specs, check_vma=False)(coefficients, vectors)

    return whole
```

```python
import functools

import jax
import jax.numpy as jnp
from jax import lax
from jax.experimental import pallas as pl
from jax.experimental.pallas import tpu as pltpu
from jax.sharding import PartitionSpec as P

MESH = pl.DeviceIdType.MESH
F32 = jnp.float32
BF16 = jnp.bfloat16
STEPS = ((-1, 0), (1, 0), (0, -1), (0, 1), (-1, -1), (-1, 1), (1, -1), (1, 1))
UP, DOWN, LEFT, RIGHT = 0, 1, 2, 3
CHUNKS = 8
SLOTS = [((m // 3 - k // 3) + 2) * 5 + (m % 3 - k % 3) + 2 for k in range(9) for m in range(9)]


RELAYS = (12, 11), (3, 4)
TURN = 7


def kernel(
    rows_total, cols_total,
    coef_hbm, v_hbm, normal_ref, image_ref,
    coef, padded, flipped, shifted, nts,
    v_vm, up_vm, down_vm, col_vm, col_out, corner_out, relay_vm,
    row_msg, col_msg, heard,
    t_hi, t_lo, w_hi, w_lo,
    load_sem, coef_sem, msg_send, msg_recv, row_send, row_recv, col_send, col_recv, cor_send, cor_recv,
    relay_recv, relay_send,
):
    gy = lax.axis_index("gy")
    gx = lax.axis_index("gx")
    ny = lax.axis_size("gy")
    nx = lax.axis_size("gx")
    rows, cols, nv = v_hbm.shape
    width = nv // CHUNKS

    def exists(n):
        dy, dx = STEPS[n]
        return (gy + dy >= 0) & (gy + dy < ny) & (gx + dx >= 0) & (gx + dx < nx)

    def at(n):
        dy, dx = STEPS[n]
        return (gy + dy, gx + dx)

    def lanes(i):
        return pl.ds(pl.multiple_of(i * width, width), width)

    def load(i):
        return pltpu.make_async_copy(v_hbm.at[:, :, lanes(i)], v_vm.at[:, :, lanes(i)], load_sem.at[i])

    def row_copy(s, i):
        src = v_hbm.at[0:2, :, lanes(i)] if s == UP else v_hbm.at[rows - 2:rows, :, lanes(i)]
        dst = down_vm if s == UP else up_vm
        return pltpu.make_async_remote_copy(
            src_ref=src, dst_ref=dst.at[:, :, lanes(i)], send_sem=row_send.at[s, i],
            recv_sem=row_recv.at[s, i], device_id=at(s), device_id_type=MESH)

    def col_copy(s, i):
        j = 2 - 2 * s
        return pltpu.make_async_remote_copy(
            src_ref=col_out.at[s, :, :, lanes(i)], dst_ref=col_vm.at[j:j + 2, 0:rows, lanes(i)],
            send_sem=col_send.at[s, i], recv_sem=col_recv.at[s, i], device_id=at(LEFT + s), device_id_type=MESH)

    turns = ((gx == TURN + 1), (gx == TURN))

    def detour(s, i):
        first, second = RELAYS[1 - s]
        via = jnp.where(i % 3 == 0, first, second)
        return pltpu.make_async_remote_copy(
            src_ref=col_out.at[s, :, :, lanes(i)], dst_ref=relay_vm.at[i // 3],
            send_sem=col_send.at[s, i], recv_sem=relay_recv.at[i // 3], device_id=(gy, via), device_id_type=MESH)

    def send_cols(s, i):
        around = turns[s] & (i % 3 < 2)
        when(exists(LEFT + s) & jnp.logical_not(around), lambda: col_copy(s, i).start())
        when(around, lambda: detour(s, i).start())

    def forward(s, i):
        j = 2 - 2 * s
        return pltpu.make_async_remote_copy(
            src_ref=relay_vm.at[i // 3], dst_ref=col_vm.at[j:j + 2, 0:rows, lanes(i)],
            send_sem=relay_send.at[i // 3], recv_sem=col_recv.at[s, i], device_id=(gy, TURN + s), device_id_type=MESH)

    def relays(f):
        for s in (0, 1):
            for n, via in enumerate(RELAYS[1 - s]):
                when(gx == via, functools.partial(f, s, n))

    def pass_on(j):
        def one(s, n):
            i = n + 3 * j
            if i < CHUNKS:
                detour(s, i).wait_recv()
                forward(s, i).start()
        relays(one)

    def passed_on(j):
        def one(s, n):
            i = n + 3 * j
            if i < CHUNKS:
                forward(s, i).wait_send()
        relays(one)

    def cor_copy(s, i):
        j = 2 - 2 * s
        return pltpu.make_async_remote_copy(
            src_ref=corner_out.at[s, :, :, lanes(i)], dst_ref=col_vm.at[j:j + 2, rows:rows + 8, lanes(i)],
            send_sem=cor_send.at[s, i], recv_sem=cor_recv.at[s, i], device_id=at(LEFT + s), device_id_type=MESH)

    def msg_copy(n):
        dy, dx = STEPS[n]
        src = row_msg.at[(dy + 1) // 2] if dy else col_msg.at[(dx + 1) // 2]
        return pltpu.make_async_remote_copy(
            src_ref=src, dst_ref=heard.at[n], send_sem=msg_send.at[n], recv_sem=msg_recv.at[n],
            device_id=at(n), device_id_type=MESH)

    opposite = [STEPS.index((-dy, -dx)) for dy, dx in STEPS]

    def when(pred, f):
        pl.when(pred)(f)

    take_coef = pltpu.make_async_copy(coef_hbm, coef, coef_sem)
    take_coef.start()
    for i in range(CHUNKS):
        load(i).start()

    barrier = pltpu.get_barrier_semaphore()
    known = jnp.int32(0)
    for n in range(8):
        when(exists(n), lambda n=n: pl.semaphore_signal(barrier, inc=1, device_id=at(n), device_id_type=MESH))
        known = known + exists(n).astype(jnp.int32)
    for side in RELAYS:
        for via in side:
            for end in (TURN, TURN + 1):
                for me, other in ((via, end), (end, via)):
                    when(gx == me, lambda other=other: pl.semaphore_signal(barrier, inc=1, device_id=(gy, other), device_id_type=MESH))
                    known = known + (gx == me).astype(jnp.int32)
    pl.semaphore_wait(barrier, known)

    def send_rows(i):
        for s in (UP, DOWN):
            when(exists(s), lambda s=s: row_copy(s, i).start())

    send_rows(0)
    padded[...] = jnp.zeros_like(padded)
    row_msg[...] = jnp.zeros_like(row_msg)
    col_msg[...] = jnp.zeros_like(col_msg)
    flipped[...] = jnp.zeros_like(flipped)
    take_coef.wait()
    padded[0:9, :, 0:cols] = coef[...]
    lane = lax.broadcasted_iota(jnp.int32, (8, 128), 1)
    for e, r in ((0, 0), (1, rows - 1)):
        for k in range(8):
            row_msg[e, k:k + 1, :] = padded[k, r:r + 1, :]
        last = pltpu.roll(jnp.broadcast_to(padded[8, r:r + 1, :], (8, 128)), 32, 1)
        row_msg[e] = jnp.where((lane >= 32) & (lane < 64), last, row_msg[e])
    for g in range(3):
        turned = padded[4 * g:4 * g + 4].reshape(128, 128).T
        col_msg[0, g:g + 1, :] = turned[0:1]
        col_msg[1, g:g + 1, :] = turned[cols - 1:cols]
        flipped[g, 1:cols + 1, :] = turned[0:cols]
    for n in range(8):
        when(exists(n), lambda n=n: msg_copy(n).start())

    def rest(i, c):
        send_rows(i)
        return c

    lax.fori_loop(1, CHUNKS, rest, 0)

    corner_out[...] = jnp.zeros_like(corner_out)

    def clear(ref):
        ref[...] = jnp.zeros_like(ref)

    when(jnp.logical_not(exists(UP)), lambda: clear(up_vm))
    when(jnp.logical_not(exists(DOWN)), lambda: clear(down_vm))
    when(jnp.logical_not(exists(LEFT)), lambda: clear(col_vm.at[0:2]))
    when(jnp.logical_not(exists(RIGHT)), lambda: clear(col_vm.at[2:4]))

    def pack(i, c):
        load(i).wait()
        for s in (0, 1):
            for j in (0, 1):
                col = j if s == 0 else cols - 2 + j
                for r in range(0, rows, 8):
                    col_out[s, j, r:r + 8, lanes(i)] = v_vm[r:r + 8, col, lanes(i)]
        for s in (0, 1):
            send_cols(s, i)
        return c

    lax.fori_loop(0, CHUNKS, pack, 0)

    for n in range(8):
        when(exists(opposite[n]), lambda n=n: msg_copy(n).wait_recv())

    def from_side(n):
        return heard[opposite[n]]

    for g in range(3):
        flipped[g, 0:1, :] = jnp.where(exists(LEFT), from_side(LEFT)[g:g + 1], 0.0)
        flipped[g, cols + 1:cols + 2, :] = jnp.where(exists(RIGHT), from_side(RIGHT)[g:g + 1], 0.0)

    def rim(side, left, right):
        out = []
        for own, a, b in ((1, 97, 33), (97, 65, 1)):
            x = jnp.where(exists(side), pltpu.roll(from_side(side), own, 1), 0.0)
            x = jnp.where((lane == 0), jnp.where(exists(left), pltpu.roll(from_side(left), a, 1), 0.0), x)
            x = jnp.where((lane == cols + 1), jnp.where(exists(right), pltpu.roll(from_side(right), b, 1), 0.0), x)
            out.append(x)
        return out

    above = rim(UP, 4, 5)
    below = rim(DOWN, 6, 7)
    er = lax.broadcasted_iota(jnp.int32, (40, 128), 0)
    ec = lax.broadcasted_iota(jnp.int32, (40, 128), 1)
    row_at = gy * rows + er - 1
    col_at = gx * cols + ec - 1
    inside = (er < rows + 2) & (ec < cols + 2) & (row_at >= 0) & (row_at < rows_total) & (col_at >= 0) & (col_at < cols_total)
    for g in range(3):
        back = flipped[g].T
        for h in range(4):
            k = 4 * g + h
            if k < 9:
                a, b = k // 3 - 1, k % 3 - 1
                shifted[0, k, 1:rows + 1, :] = back[32 * h:32 * h + rows]
                which, line = (0, k) if k < 8 else (1, 0)
                shifted[0, k, 0:1, :] = above[which][line:line + 1]
                shifted[0, k, rows + 1:rows + 2, :] = below[which][line:line + 1]
                keep = inside & (row_at + a >= 0) & (row_at + a < rows_total) & (col_at + b >= 0) & (col_at + b < cols_total)
                x = jnp.where(keep, shifted[0, k], 0.0)
                shifted[0, k] = x
                shifted[1, k] = pltpu.roll(x, 127, 1)
                shifted[2, k] = pltpu.roll(x, 126, 1)
    terms = []
    for slot in range(25):
        total = None
        for at_pair in range(81):
            if SLOTS[at_pair] == slot:
                k, m = at_pair // 9, at_pair % 9
                a, b = k // 3 - 1, k % 3 - 1
                term = shifted[1 - b, k, 1 - a:1 - a + rows, :] * shifted[1 - b, m, 1 - a:1 - a + rows, :]
                total = term if total is None else total + term
        normal_ref[slot] = total[:, 0:cols]
        terms.append(total)
    for g in range(7):
        group = terms[4 * g:4 * g + 4]
        while len(group) < 4:
            group.append(jnp.zeros_like(group[0]))
        turned = jnp.concatenate(group, axis=0).T[0:cols]
        nts[0, g] = turned
        for b in range(1, 4):
            nts[b, g] = pltpu.roll(turned, 128 - 8 * b, 1)

    lane32 = lax.broadcasted_iota(jnp.int32, (cols, 128), 1)
    cell = lax.broadcasted_iota(jnp.int32, (cols, 128), 0)
    own_at, side_at = {}, {}
    for f in range(-2, 3):
        t = cell + f
        own_at[f] = jnp.where((t >= 0) & (t < cols), t, -1000)
        side_at[f] = jnp.where(t == -2, 0, jnp.where(t == -1, 32, jnp.where(t == cols, 64, jnp.where(t == cols + 1, 96, -1000))))

    def build(b, c):
        for rl in range(8):
            own = [jnp.zeros((cols, 128), F32) for _ in range(3)]
            side = jnp.zeros((cols, 128), F32)
            for e in range(-2, 3):
                spot = rl + e + 2
                tile, q = spot // 4, spot % 4
                row = b * 8 + rl + e
                slot = jnp.where(row < 0, 18 + row, row)
                slot = jnp.where(b == 3, jnp.where(row < rows, row - 16, row - 14), slot)
                for f in range(-2, 3):
                    index = (e + 2) * 5 + f + 2
                    at_lane = (index % 4) * 32 + rl
                    column = jnp.broadcast_to(nts[b, index // 4][:, at_lane:at_lane + 1], (cols, 128))
                    own[tile] = jnp.where(lane32 - 32 * q == own_at[f], column, own[tile])
                    if f:
                        side = jnp.where(lane32 - slot == side_at[f], column, side)
            for tile, x in enumerate(own + [side]):
                hi = x.astype(BF16)
                t_hi[b, rl * 32:rl * 32 + 32, tile * 128:tile * 128 + 128] = hi
                t_lo[b, rl * 32:rl * 32 + 32, tile * 128:tile * 128 + 128] = (x - hi.astype(F32)).astype(BF16)
        return c

    pass_on(0)
    lax.fori_loop(0, 2, build, 0)
    pass_on(1)
    lax.fori_loop(2, 4, build, 0)
    pass_on(2)

    def halves(x):
        hi = x.astype(BF16)
        return hi, (x - hi.astype(F32)).astype(BF16)

    def put(block, start, hi, lo):
        w_hi[block, start:start + hi.shape[0], :] = hi
        w_lo[block, start:start + hi.shape[0], :] = lo

    def compute(i):
        at_i = lanes(i)
        for s in (0, 1):
            when(exists(LEFT + 1 - s), lambda s=s: (col_copy(s, i).wait_recv(), cor_copy(s, i).wait_recv())[0])
        for q in range(4):
            hi, lo = halves(v_vm[8 * q:8 * q + 8, :, at_i].reshape(256, width))
            put(q, 64, hi, lo)
            if q > 0:
                put(q - 1, 320, hi[0:64], lo[0:64])
            if q < 3:
                put(q + 1, 0, hi[192:256], lo[192:256])
        put(0, 0, *halves(up_vm[:, :, at_i].reshape(64, width)))
        put(3, 320, *halves(down_vm[:, :, at_i].reshape(64, width)))
        for j in range(4):
            hi, lo = halves(col_vm[j, 0:32, at_i])
            chi, clo = halves(jnp.concatenate([col_vm[j, 32:40, at_i], jnp.zeros((8, width), F32)], axis=0))
            put(0, 384 + 32 * j, hi[0:16], lo[0:16])
            put(0, 400 + 32 * j, chi, clo)
            put(1, 384 + 32 * j, hi, lo)
            put(2, 384 + 32 * j, hi, lo)
            put(3, 384 + 32 * j, hi[16:32], lo[16:32])
            put(3, 400 + 32 * j, chi, clo)
        for q in range(4):
            y = jnp.dot(t_hi[q], w_hi[q], preferred_element_type=F32)
            y = y + jnp.dot(t_lo[q], w_hi[q], preferred_element_type=F32)
            y = y + jnp.dot(t_hi[q], w_lo[q], preferred_element_type=F32)
            image_ref[8 * q:8 * q + 8, :, at_i] = y.reshape(8, cols, width)

    def main(i, c):
        for s in (UP, DOWN):
            when(exists(1 - s), lambda s=s: row_copy(s, i).wait_recv())
        for s in (0, 1):
            for j in (0, 1):
                col = j if s == 0 else cols - 2 + j
                for h in (0, 1):
                    corner_out[s, j, h:h + 1, lanes(i)] = up_vm[h, col:col + 1, lanes(i)]
                    corner_out[s, j, 2 + h:3 + h, lanes(i)] = down_vm[h, col:col + 1, lanes(i)]
            when(exists(LEFT + s), lambda s=s: cor_copy(s, i).start())
        when(i > 0, lambda: compute(i - 1))
        return c

    lax.fori_loop(0, CHUNKS, main, 0)
    compute(CHUNKS - 1)

    def finish(i, c):
        for s in (0, 1):
            when(exists(s), lambda s=s: row_copy(s, i).wait_send())
            when(exists(LEFT + s), lambda s=s: (col_copy(s, i).wait_send(), cor_copy(s, i).wait_send())[0])
        return c

    lax.fori_loop(0, CHUNKS, finish, 0)
    for n in range(8):
        when(exists(n), lambda n=n: msg_copy(n).wait_send())
    for j in range(3):
        passed_on(j)


def per_device(rows_total, cols_total, coefficients, vectors):
    _, rows, cols = coefficients.shape
    nv = vectors.shape[2]
    width = nv // CHUNKS
    dma = pltpu.SemaphoreType.DMA
    return pl.pallas_call(
        functools.partial(kernel, rows_total, cols_total),
        out_shape=(pltpu.VMEM((25, rows, cols), F32), pltpu.VMEM((rows, cols, nv), F32)),
        in_specs=[pl.BlockSpec(memory_space=pltpu.HBM)] * 2,
        out_specs=(pl.BlockSpec(memory_space=pltpu.VMEM),) * 2,
        scratch_shapes=[
            pltpu.VMEM((9, rows, cols), F32),
            pltpu.VMEM((12, rows, 128), F32),
            pltpu.VMEM((3, 128, 128), F32),
            pltpu.VMEM((3, 9, 40, 128), F32),
            pltpu.VMEM((4, 7, cols, 128), F32),
            pltpu.VMEM((rows, cols, nv), F32),
            pltpu.VMEM((2, cols, nv), F32),
            pltpu.VMEM((2, cols, nv), F32),
            pltpu.VMEM((4, rows + 8, nv), F32),
            pltpu.VMEM((2, 2, rows, nv), F32),
            pltpu.VMEM((2, 2, 8, nv), F32),
            pltpu.VMEM((3, 2, rows, width), F32),
            pltpu.VMEM((2, 8, 128), F32),
            pltpu.VMEM((2, 8, 128), F32),
            pltpu.VMEM((8, 8, 128), F32),
            pltpu.VMEM((4, 256, 512), BF16),
            pltpu.VMEM((4, 256, 512), BF16),
            pltpu.VMEM((4, 512, width), BF16),
            pltpu.VMEM((4, 512, width), BF16),
            dma((CHUNKS,)), dma,
            dma((8,)), dma((8,)),
            dma((2, CHUNKS)), dma((2, CHUNKS)),
            dma((2, CHUNKS)), dma((2, CHUNKS)),
            dma((2, CHUNKS)), dma((2, CHUNKS)),
            dma((3,)), dma((3,)),
        ],
        compiler_params=pltpu.CompilerParams(collective_id=0, has_side_effects=True, vmem_limit_bytes=44 * 2**20),
    )(coefficients, vectors)


def solution(mesh):
    in_specs = (P(None, "gy", "gx"), P("gy", "gx", None))
    out_specs = (P(None, "gy", "gx"), P("gy", "gx", None))

    def whole(coefficients, vectors):
        body = functools.partial(per_device, coefficients.shape[1], coefficients.shape[2])
        return jax.shard_map(body, mesh=mesh, in_specs=in_specs, out_specs=out_specs, check_vma=False)(coefficients, vectors)

    return whole
```

```python
import functools

import jax
import jax.numpy as jnp
from jax import lax
from jax.experimental import pallas as pl
from jax.experimental.pallas import tpu as pltpu
from jax.sharding import PartitionSpec as P

MESH = pl.DeviceIdType.MESH
F32 = jnp.float32
BF16 = jnp.bfloat16
STEPS = ((-1, 0), (1, 0), (0, -1), (0, 1), (-1, -1), (-1, 1), (1, -1), (1, 1))
UP, DOWN, LEFT, RIGHT = 0, 1, 2, 3
CHUNKS = 8
GROUP = 4
SETS = 3
LEFT_OVER = 2
SLOTS = [((m // 3 - k // 3) + 2) * 5 + (m % 3 - k % 3) + 2 for k in range(9) for m in range(9)]


RELAYS = (12, 11), (3, 4)
TURN = 7


def kernel(
    rows_total, cols_total,
    coef_hbm, v_hbm, normal_ref, image_ref, t_hi, t_lo, w_hi, w_lo,
    coef, padded, flipped, shifted, nts,
    v_vm, up_vm, down_vm, col_vm, col_out, corner_out, relay_vm, hop_vm, diag_out, diag_vm,
    row_msg, col_msg, heard,
    load_sem, coef_sem, msg_send, msg_recv, row_send, row_recv, col_send, col_recv, cor_send, cor_recv,
    relay_recv, relay_send, hop_recv, hop_send, diag_send, diag_recv,
):
    gy = lax.axis_index("gy")
    gx = lax.axis_index("gx")
    ny = lax.axis_size("gy")
    nx = lax.axis_size("gx")
    rows, cols, nv = v_hbm.shape
    width = nv // CHUNKS

    def exists(n):
        dy, dx = STEPS[n]
        return (gy + dy >= 0) & (gy + dy < ny) & (gx + dx >= 0) & (gx + dx < nx)

    def at(n):
        dy, dx = STEPS[n]
        return (gy + dy, gx + dx)

    def lanes(i):
        return pl.ds(pl.multiple_of(i * width, width), width)

    def span(n):
        return pl.ds(0, n * width)

    def load(part):
        return pltpu.make_async_copy(v_hbm.at[part], v_vm.at[part], load_sem)

    def row_copy(s, i):
        src = v_hbm.at[0:2, :, lanes(i)] if s == UP else v_hbm.at[rows - 2:rows, :, lanes(i)]
        dst = down_vm if s == UP else up_vm
        return pltpu.make_async_remote_copy(
            src_ref=src, dst_ref=dst.at[:, :, lanes(i)], send_sem=row_send.at[s],
            recv_sem=row_recv.at[s, i], device_id=at(s), device_id_type=MESH)

    odd = gy % 2 == 1
    plane = gy // 2
    crossing = (jnp.logical_not(odd), odd)
    late = jnp.where(odd, 2 * plane + 2, CHUNKS - 2 * plane)
    held = jnp.where(odd, 2 * plane, jnp.maximum(CHUNKS - 2 - 2 * plane, 0))

    def hop(s, i, count):
        src = v_hbm.at[0:2, :, lanes(i)] if s == UP else v_hbm.at[rows - 2:rows, :, lanes(i)]
        slot = i - CHUNKS + count
        return pltpu.make_async_remote_copy(
            src_ref=src, dst_ref=hop_vm.at[slot], send_sem=row_send.at[s], recv_sem=hop_recv.at[slot],
            device_id=(gy + (2 if s == DOWN else -2), gx), device_id_type=MESH)

    def send_rows(i):
        for s in (UP, DOWN):
            detoured = crossing[s] & (i >= CHUNKS - late)
            when(exists(s) & jnp.logical_not(detoured), lambda s=s: row_copy(s, i).start())
            when(exists(s) & detoured, lambda s=s: hop(s, i, late).start())

    def hop_on(s, slot):
        i = CHUNKS - held + slot
        return pltpu.make_async_remote_copy(
            src_ref=hop_vm.at[slot], dst_ref=(down_vm if s == UP else up_vm).at[:, :, lanes(i)],
            send_sem=hop_send.at[slot], recv_sem=row_recv.at[s, i],
            device_id=(gy + (1 if s == UP else -1), gx), device_id_type=MESH)

    def each_held(slots, f):
        for s in (UP, DOWN):
            for slot in slots:
                when(crossing[s] & (slot < held), functools.partial(f, s, slot))

    def hop_pass(s, slot):
        hop(s, CHUNKS - held + slot, held).wait_recv()
        hop_on(s, slot).start()

    def col_copy(s, i):
        j = 2 - 2 * s
        return pltpu.make_async_remote_copy(
            src_ref=col_out.at[s, :, :, lanes(i)], dst_ref=col_vm.at[j:j + 2, 0:rows, lanes(i)],
            send_sem=col_send.at[s], recv_sem=col_recv.at[s, i // GROUP], device_id=at(LEFT + s), device_id_type=MESH)

    turns = ((gx == TURN + 1), (gx == TURN))

    def detour(s, i):
        first, second = RELAYS[1 - s]
        via = jnp.where(i % 3 == 0, first, second)
        return pltpu.make_async_remote_copy(
            src_ref=col_out.at[s, :, :, lanes(i)], dst_ref=relay_vm.at[i // 3],
            send_sem=col_send.at[s], recv_sem=relay_recv.at[i // 3], device_id=(gy, via), device_id_type=MESH)

    def send_cols(s, i):
        around = turns[s] & (i % 3 < 2)
        when(exists(LEFT + s) & jnp.logical_not(around), lambda: col_copy(s, i).start())
        when(around, lambda: detour(s, i).start())

    def forward(s, i):
        j = 2 - 2 * s
        return pltpu.make_async_remote_copy(
            src_ref=relay_vm.at[i // 3], dst_ref=col_vm.at[j:j + 2, 0:rows, lanes(i)],
            send_sem=relay_send.at[i // 3], recv_sem=col_recv.at[s, i // GROUP], device_id=(gy, TURN + s), device_id_type=MESH)

    def relays(f):
        for s in (0, 1):
            for n, via in enumerate(RELAYS[1 - s]):
                when(gx == via, functools.partial(f, s, n))

    def pass_on(j):
        def one(s, n):
            i = n + 3 * j
            if i < CHUNKS:
                detour(s, i).wait_recv()
                forward(s, i).start()
        relays(one)

    def passed_on(j):
        def one(s, n):
            i = n + 3 * j
            if i < CHUNKS:
                forward(s, i).wait_send()
        relays(one)

    def cor_copy(s, i):
        j = 2 - 2 * s
        return pltpu.make_async_remote_copy(
            src_ref=corner_out.at[s, :, :, lanes(i)], dst_ref=col_vm.at[j:j + 2, rows:rows + 8, lanes(i)],
            send_sem=cor_send.at[s], recv_sem=cor_recv.at[s, i], device_id=at(LEFT + s), device_id_type=MESH)

    def msg_copy(n):
        dy, dx = STEPS[n]
        src = row_msg.at[(dy + 1) // 2] if dy else col_msg.at[(dx + 1) // 2]
        return pltpu.make_async_remote_copy(
            src_ref=src, dst_ref=heard.at[n], send_sem=msg_send, recv_sem=msg_recv,
            device_id=at(n), device_id_type=MESH)

    def diag_copy(n):
        return pltpu.make_async_remote_copy(
            src_ref=diag_out.at[n - 4], dst_ref=diag_vm.at[n - 4], send_sem=diag_send.at[n - 4],
            recv_sem=diag_recv.at[n - 4], device_id=at(n), device_id_type=MESH)

    opposite = [STEPS.index((-dy, -dx)) for dy, dx in STEPS]

    def when(pred, f):
        pl.when(pred)(f)

    take_coef = pltpu.make_async_copy(coef_hbm, coef, coef_sem)
    barrier = pltpu.get_barrier_semaphore()
    take_coef.start()
    known = jnp.int32(0)
    for n in range(8):
        when(exists(n), lambda n=n: pl.semaphore_signal(barrier, inc=1, device_id=at(n), device_id_type=MESH))
        known = known + exists(n).astype(jnp.int32)
    for dy in (-2, 2):
        there = (gy + dy >= 0) & (gy + dy < ny)
        when(there, lambda dy=dy: pl.semaphore_signal(barrier, inc=1, device_id=(gy + dy, gx), device_id_type=MESH))
        known = known + there.astype(jnp.int32)
    for side in RELAYS:
        for via in side:
            for end in (TURN, TURN + 1):
                for me, other in ((via, end), (end, via)):
                    when(gx == me, lambda other=other: pl.semaphore_signal(barrier, inc=1, device_id=(gy, other), device_id_type=MESH))
                    known = known + (gx == me).astype(jnp.int32)
    padded[...] = jnp.zeros_like(padded)
    row_msg[...] = jnp.zeros_like(row_msg)
    col_msg[...] = jnp.zeros_like(col_msg)
    flipped[...] = jnp.zeros_like(flipped)
    take_coef.wait()
    for q in range(4):
        load(pl.ds(8 * q, 8)).start()
    padded[0:9, :, 0:cols] = coef[...]
    lane = lax.broadcasted_iota(jnp.int32, (8, 128), 1)
    for e, r in ((0, 0), (1, rows - 1)):
        for k in range(8):
            row_msg[e, k:k + 1, :] = padded[k, r:r + 1, :]
        last = pltpu.roll(jnp.broadcast_to(padded[8, r:r + 1, :], (8, 128)), 32, 1)
        row_msg[e] = jnp.where((lane >= 32) & (lane < 64), last, row_msg[e])
    for g in range(3):
        turned = padded[4 * g:4 * g + 4].reshape(128, 128).T
        col_msg[0, g:g + 1, :] = turned[0:1]
        col_msg[1, g:g + 1, :] = turned[cols - 1:cols]
        flipped[g, 1:cols + 1, :] = turned[0:cols]
    pl.semaphore_wait(barrier, known)

    for n in range(8):
        when(exists(n), lambda n=n: msg_copy(n).start())

    def rest(i, c):
        send_rows(i)
        return c

    lax.fori_loop(0, CHUNKS, rest, 0)

    corner_out[...] = jnp.zeros_like(corner_out)

    def clear(ref):
        ref[...] = jnp.zeros_like(ref)

    when(jnp.logical_not(exists(UP)), lambda: clear(up_vm))
    when(jnp.logical_not(exists(DOWN)), lambda: clear(down_vm))
    when(jnp.logical_not(exists(LEFT)), lambda: clear(col_vm.at[0:2]))
    when(jnp.logical_not(exists(RIGHT)), lambda: clear(col_vm.at[2:4]))

    def pack(i, c):
        for s in (0, 1):
            for j in (0, 1):
                col = j if s == 0 else cols - 2 + j
                for r in range(0, rows, 8):
                    col_out[s, j, r:r + 8, lanes(i)] = v_vm[r:r + 8, col, lanes(i)]
        for s in (0, 1):
            send_cols(s, i)
        return c

    load(pl.ds(0, rows)).wait()
    lax.fori_loop(0, CHUNKS, pack, 0)
    for n in range(4, 8):
        dy, dx = STEPS[n]
        for c in (0, 1):
            for h in (0, 1):
                row, col = (h if dy < 0 else rows - 2 + h), (c if dx < 0 else cols - 2 + c)
                diag_out[n - 4, 2 * c + h:2 * c + h + 1, :] = v_vm[row, col:col + 1, lanes(CHUNKS - 1)]
        when(exists(n), lambda n=n: diag_copy(n).start())
        when(jnp.logical_not(exists(opposite[n])), lambda n=n: clear(diag_vm.at[n - 4]))

    def sent(ref, sem):
        pltpu.make_async_copy(ref, ref, sem).wait()

    neighbours = jnp.int32(0)
    for n in range(8):
        neighbours = neighbours + exists(n).astype(jnp.int32)

    def messages(sem):
        for n in (3, 5, 8):
            when(neighbours == n, lambda n=n: sent(heard.at[0:n], sem))

    messages(msg_recv)

    def from_side(n):
        return heard[opposite[n]]

    for g in range(3):
        flipped[g, 0:1, :] = jnp.where(exists(LEFT), from_side(LEFT)[g:g + 1], 0.0)
        flipped[g, cols + 1:cols + 2, :] = jnp.where(exists(RIGHT), from_side(RIGHT)[g:g + 1], 0.0)

    def rim(side, left, right):
        out = []
        for own, a, b in ((1, 97, 33), (97, 65, 1)):
            x = jnp.where(exists(side), pltpu.roll(from_side(side), own, 1), 0.0)
            x = jnp.where((lane == 0), jnp.where(exists(left), pltpu.roll(from_side(left), a, 1), 0.0), x)
            x = jnp.where((lane == cols + 1), jnp.where(exists(right), pltpu.roll(from_side(right), b, 1), 0.0), x)
            out.append(x)
        return out

    above = rim(UP, 4, 5)
    below = rim(DOWN, 6, 7)
    er = lax.broadcasted_iota(jnp.int32, (40, 128), 0)
    ec = lax.broadcasted_iota(jnp.int32, (40, 128), 1)
    row_at = gy * rows + er - 1
    col_at = gx * cols + ec - 1
    inside = (er < rows + 2) & (ec < cols + 2) & (row_at >= 0) & (row_at < rows_total) & (col_at >= 0) & (col_at < cols_total)
    for g in range(3):
        back = flipped[g].T
        for h in range(4):
            k = 4 * g + h
            if k < 9:
                a, b = k // 3 - 1, k % 3 - 1
                shifted[0, k, 1:rows + 1, :] = back[32 * h:32 * h + rows]
                which, line = (0, k) if k < 8 else (1, 0)
                shifted[0, k, 0:1, :] = above[which][line:line + 1]
                shifted[0, k, rows + 1:rows + 2, :] = below[which][line:line + 1]
                keep = inside & (row_at + a >= 0) & (row_at + a < rows_total) & (col_at + b >= 0) & (col_at + b < cols_total)
                x = jnp.where(keep, shifted[0, k], 0.0)
                shifted[0, k] = x
                shifted[1, k] = pltpu.roll(x, 127, 1)
                shifted[2, k] = pltpu.roll(x, 126, 1)
    terms = []
    for slot in range(25):
        total = None
        for at_pair in range(81):
            if SLOTS[at_pair] == slot:
                k, m = at_pair // 9, at_pair % 9
                a, b = k // 3 - 1, k % 3 - 1
                term = shifted[1 - b, k, 1 - a:1 - a + rows, :] * shifted[1 - b, m, 1 - a:1 - a + rows, :]
                total = term if total is None else total + term
        normal_ref[slot] = total[:, 0:cols]
        terms.append(total)
    for g in range(7):
        group = terms[4 * g:4 * g + 4]
        while len(group) < 4:
            group.append(jnp.zeros_like(group[0]))
        turned = jnp.concatenate(group, axis=0).T[0:cols]
        nts[0, g] = turned
        for b in range(1, 4):
            nts[b, g] = pltpu.roll(turned, 128 - 8 * b, 1)

    lane32 = lax.broadcasted_iota(jnp.int32, (cols, 128), 1)
    cell = lax.broadcasted_iota(jnp.int32, (cols, 128), 0)
    own_at, side_at = {}, {}
    for f in range(-2, 3):
        t = cell + f
        own_at[f] = jnp.where((t >= 0) & (t < cols), t, -1000)
        side_at[f] = jnp.where(t == -2, 0, jnp.where(t == -1, 32, jnp.where(t == cols, 64, jnp.where(t == cols + 1, 96, -1000))))

    def build(b, c):
        for rl in range(8):
            own = [jnp.zeros((cols, 128), F32) for _ in range(3)]
            side = jnp.zeros((cols, 128), F32)
            for e in range(-2, 3):
                spot = rl + e + 2
                tile, q = spot // 4, spot % 4
                row = b * 8 + rl + e
                slot = jnp.where(row < 0, 18 + row, row)
                slot = jnp.where(b == 3, jnp.where(row < rows, row - 16, row - 14), slot)
                for f in range(-2, 3):
                    index = (e + 2) * 5 + f + 2
                    at_lane = (index % 4) * 32 + rl
                    column = jnp.broadcast_to(nts[b, index // 4][:, at_lane:at_lane + 1], (cols, 128))
                    own[tile] = jnp.where(lane32 - 32 * q == own_at[f], column, own[tile])
                    if f:
                        side = jnp.where(lane32 - slot == side_at[f], column, side)
            for tile, x in enumerate(own + [side]):
                hi = x.astype(BF16)
                t_hi[b, rl * 32:rl * 32 + 32, tile * 128:tile * 128 + 128] = hi
                t_lo[b, rl * 32:rl * 32 + 32, tile * 128:tile * 128 + 128] = (x - hi.astype(F32)).astype(BF16)
        return c

    lax.fori_loop(0, 2, build, 0)
    pass_on(0)
    each_held((0, 1), hop_pass)
    lax.fori_loop(2, 4, build, 0)
    pass_on(1)
    each_held((2,), hop_pass)

    def halves(x):
        hi = x.astype(BF16)
        return hi, (x - hi.astype(F32)).astype(BF16)

    def put(i, block, start, hi, lo):
        w_hi[i % SETS, block, start:start + hi.shape[0], :] = hi
        w_lo[i % SETS, block, start:start + hi.shape[0], :] = lo

    def own_part(i):
        for q in range(4):
            hi, lo = halves(v_vm[8 * q:8 * q + 8, :, lanes(i)].reshape(256, width))
            put(i, q, 64, hi, lo)
            if q > 0:
                put(i, q - 1, 320, hi[0:64], lo[0:64])
            if q < 3:
                put(i, q + 1, 0, hi[192:256], lo[192:256])

    def side_part(i, last=False):
        def columns(s):
            j = 2 - 2 * s
            at_group = pl.ds(pl.multiple_of(i * width, width), GROUP * width)
            whole = col_vm.at[j:j + 2, 0:rows, at_group]
            pltpu.make_async_copy(whole, whole, col_recv.at[s, i // GROUP]).wait()

        for s in (0, 1):
            if not last:
                when(exists(LEFT + 1 - s) & (i % GROUP == 0), functools.partial(columns, s))
                when(exists(LEFT + 1 - s), lambda s=s: cor_copy(s, i).wait_recv())
        if last:
            for n in range(4, 8):
                when(exists(opposite[n]), lambda n=n: diag_copy(n).wait_recv())
        for j in range(4):
            hi, lo = halves(col_vm[j, 0:32, lanes(i)])
            if last:
                from_above, from_below = (6, 4) if j >= 2 else (7, 5)
                c = 2 * (j % 2)
                corner = jnp.concatenate([
                    diag_vm[from_above - 4, c:c + 2, :], diag_vm[from_below - 4, c:c + 2, :], jnp.zeros((12, width), F32)], axis=0)
            else:
                corner = jnp.concatenate([col_vm[j, 32:40, lanes(i)], jnp.zeros((8, width), F32)], axis=0)
            chi, clo = halves(corner)
            put(i, 0, 384 + 32 * j, hi[0:16], lo[0:16])
            put(i, 0, 400 + 32 * j, chi, clo)
            put(i, 1, 384 + 32 * j, hi, lo)
            put(i, 2, 384 + 32 * j, hi, lo)
            put(i, 3, 384 + 32 * j, hi[16:32], lo[16:32])
            put(i, 3, 400 + 32 * j, chi, clo)

    def compute(i):
        side_part(i)
        for q in range(4):
            y = products(t_hi[q], t_lo[q], w_hi[i % SETS, q], w_lo[i % SETS, q])
            image_ref[8 * q:8 * q + 8, :, lanes(i)] = y.reshape(8, cols, width)

    def main(i, c):
        for step, slots in ((1, (3,)), (2, (4,)), (3, (5,))):
            when(i == step, lambda slots=slots: each_held(slots, hop_pass))
        when(i == 2, lambda: pass_on(2))
        own_part(i)
        when(i > 1, lambda: compute(i - 2))
        for s in (UP, DOWN):
            when(exists(1 - s), lambda s=s: row_copy(s, i).wait_recv())
        for s in (0, 1):
            for j in (0, 1):
                col = j if s == 0 else cols - 2 + j
                for h in (0, 1):
                    corner_out[s, j, h:h + 1, lanes(i)] = up_vm[h, col:col + 1, lanes(i)]
                    corner_out[s, j, 2 + h:3 + h, lanes(i)] = down_vm[h, col:col + 1, lanes(i)]
            when(exists(LEFT + s) & (i < CHUNKS - 1), lambda s=s: cor_copy(s, i).start())
        put(i, 0, 0, *halves(up_vm[:, :, lanes(i)].reshape(64, width)))
        put(i, 3, 320, *halves(down_vm[:, :, lanes(i)].reshape(64, width)))
        return c

    lax.fori_loop(0, CHUNKS, main, 0)
    side_part(CHUNKS - 2)
    side_part(CHUNKS - 1, last=True)

    for s in (0, 1):
        when(exists(s), lambda s=s: sent(up_vm, row_send.at[s]))
        when(exists(LEFT + s), lambda s=s: sent(col_out.at[s], col_send.at[s]))
        when(exists(LEFT + s), lambda s=s: sent(corner_out.at[s, :, :, span(CHUNKS - 1)], cor_send.at[s]))
    for n in range(4, 8):
        when(exists(n), lambda n=n: diag_copy(n).wait_send())
    messages(msg_send)
    for j in range(3):
        passed_on(j)
    each_held(range(6), lambda s, slot: hop_on(s, slot).wait_send())


def products(t_hi, t_lo, w_hi, w_lo):
    y = jnp.dot(t_hi, w_hi, preferred_element_type=F32)
    y = y + jnp.dot(t_lo, w_hi, preferred_element_type=F32)
    return y + jnp.dot(t_hi, w_lo, preferred_element_type=F32)


def last_chunks(normal_vm, image_vm, t_hi, t_lo, w_hi, w_lo, normal_hbm, image_hbm, tail, normal_sem, image_sem, tail_sem):
    rows, cols, nv = image_hbm.shape
    width = nv // CHUNKS
    done = nv - LEFT_OVER * width
    copies = [pltpu.make_async_copy(
        image_vm.at[8 * q:8 * q + 8, :, :], image_hbm.at[8 * q:8 * q + 8, :, 0:done], image_sem.at[q]) for q in range(4)]
    copies.append(pltpu.make_async_copy(normal_vm, normal_hbm, normal_sem))
    for copy in copies:
        copy.start()
    for n in range(LEFT_OVER):
        i = CHUNKS - LEFT_OVER + n
        for q in range(4):
            y = products(t_hi[q], t_lo[q], w_hi[i % SETS, q], w_lo[i % SETS, q])
            tail[n, q] = y.reshape(8, cols, width)
            copies.append(pltpu.make_async_copy(
                tail.at[n, q], image_hbm.at[8 * q:8 * q + 8, :, i * width:i * width + width], tail_sem.at[n, q]))
            copies[-1].start()
    for copy in copies:
        copy.wait()


def per_device(rows_total, cols_total, coefficients, vectors):
    _, rows, cols = coefficients.shape
    nv = vectors.shape[2]
    width = nv // CHUNKS
    dma = pltpu.SemaphoreType.DMA
    parts = pl.pallas_call(
        functools.partial(kernel, rows_total, cols_total),
        out_shape=(
            pltpu.VMEM((25, rows, cols), F32), pltpu.VMEM((rows, cols, nv - LEFT_OVER * width), F32),
            pltpu.VMEM((4, 256, 512), BF16), pltpu.VMEM((4, 256, 512), BF16),
            pltpu.VMEM((SETS, 4, 512, width), BF16), pltpu.VMEM((SETS, 4, 512, width), BF16)),
        in_specs=[pl.BlockSpec(memory_space=pltpu.HBM)] * 2,
        out_specs=(pl.BlockSpec(memory_space=pltpu.VMEM),) * 6,
        scratch_shapes=[
            pltpu.VMEM((9, rows, cols), F32),
            pltpu.VMEM((12, rows, 128), F32),
            pltpu.VMEM((3, 128, 128), F32),
            pltpu.VMEM((3, 9, 40, 128), F32),
            pltpu.VMEM((4, 7, cols, 128), F32),
            pltpu.VMEM((rows, cols, nv), F32),
            pltpu.VMEM((2, cols, nv), F32),
            pltpu.VMEM((2, cols, nv), F32),
            pltpu.VMEM((4, rows + 8, nv), F32),
            pltpu.VMEM((2, 2, rows, nv), F32),
            pltpu.VMEM((2, 2, 8, nv), F32),
            pltpu.VMEM((3, 2, rows, width), F32),
            pltpu.VMEM((6, 2, cols, width), F32),
            pltpu.VMEM((4, 4, width), F32),
            pltpu.VMEM((4, 4, width), F32),
            pltpu.VMEM((2, 8, 128), F32),
            pltpu.VMEM((2, 8, 128), F32),
            pltpu.VMEM((8, 8, 128), F32),
            dma, dma,
            dma, dma,
            dma((2,)), dma((2, CHUNKS)),
            dma((2,)), dma((2, CHUNKS // GROUP)),
            dma((2,)), dma((2, CHUNKS - 1)),
            dma((3,)), dma((3,)),
            dma((6,)), dma((6,)),
            dma((4,)), dma((4,)),
        ],
        compiler_params=pltpu.CompilerParams(collective_id=0, has_side_effects=True, vmem_limit_bytes=44 * 2**20),
    )(pltpu.with_memory_space_constraint(coefficients, pltpu.HBM), vectors)
    return pl.pallas_call(
        last_chunks,
        out_shape=(jax.ShapeDtypeStruct((25, rows, cols), F32), jax.ShapeDtypeStruct((rows, cols, nv), F32)),
        in_specs=[pl.BlockSpec(memory_space=pltpu.VMEM)] * 6,
        out_specs=(pl.BlockSpec(memory_space=pltpu.HBM),) * 2,
        scratch_shapes=[pltpu.VMEM((LEFT_OVER, 4, 8, cols, width), F32), dma, dma((4,)), dma((LEFT_OVER, 4))],
        compiler_params=pltpu.CompilerParams(vmem_limit_bytes=8 * 2**20),
    )(*parts)


def solution(mesh):
    in_specs = (P(None, "gy", "gx"), P("gy", "gx", None))
    out_specs = (P(None, "gy", "gx"), P("gy", "gx", None))

    def whole(coefficients, vectors):
        body = functools.partial(per_device, coefficients.shape[1], coefficients.shape[2])
        return jax.shard_map(body, mesh=mesh, in_specs=in_specs, out_specs=out_specs, check_vma=False)(coefficients, vectors)

    return whole
```

```python
import functools

import jax
import jax.numpy as jnp
from jax import lax
from jax.experimental import pallas as pl
from jax.experimental.pallas import tpu as pltpu
from jax.sharding import PartitionSpec as P

MESH = pl.DeviceIdType.MESH
F32 = jnp.float32
BF16 = jnp.bfloat16
STEPS = ((-1, 0), (1, 0), (0, -1), (0, 1), (-1, -1), (-1, 1), (1, -1), (1, 1))
UP, DOWN, LEFT, RIGHT = 0, 1, 2, 3
CHUNKS = 8
GROUP = 4
LAG = 3
SETS = LAG + 1
SLOTS = [((m // 3 - k // 3) + 2) * 5 + (m % 3 - k % 3) + 2 for k in range(9) for m in range(9)]


RELAYS = (12, 11), (3, 4)
TURN = 7


def kernel(
    rows_total, cols_total,
    coef_hbm, v_hbm, normal_ref, image_ref, t_hi, t_lo, w_hi, w_lo,
    coef, padded, flipped, shifted, nts,
    v_vm, up_vm, down_vm, col_vm, col_out, corner_out, corner_vm, relay_vm, hop_vm, diag_out, diag_vm,
    row_msg, col_msg, heard,
    load_sem, coef_sem, msg_send, msg_recv, row_send, row_recv, col_send, col_recv, cor_send, cor_recv,
    relay_recv, relay_send, hop_recv, hop_send, diag_send, diag_recv,
):
    gy = lax.axis_index("gy")
    gx = lax.axis_index("gx")
    ny = lax.axis_size("gy")
    nx = lax.axis_size("gx")
    rows, cols, nv = v_hbm.shape
    width = nv // CHUNKS

    def exists(n):
        dy, dx = STEPS[n]
        return (gy + dy >= 0) & (gy + dy < ny) & (gx + dx >= 0) & (gx + dx < nx)

    def at(n):
        dy, dx = STEPS[n]
        return (gy + dy, gx + dx)

    def lanes(i):
        return pl.ds(pl.multiple_of(i * width, width), width)

    def span(n):
        return pl.ds(0, n * width)

    def load(part):
        return pltpu.make_async_copy(v_hbm.at[part], v_vm.at[part], load_sem)

    def row_copy(s, i):
        src = v_hbm.at[0:2, :, lanes(i)] if s == UP else v_hbm.at[rows - 2:rows, :, lanes(i)]
        dst = down_vm if s == UP else up_vm
        return pltpu.make_async_remote_copy(
            src_ref=src, dst_ref=dst.at[:, :, lanes(i)], send_sem=row_send.at[s],
            recv_sem=row_recv.at[s, i], device_id=at(s), device_id_type=MESH)

    odd = gy % 2 == 1
    plane = gy // 2
    crossing = (jnp.logical_not(odd), odd)
    late = jnp.where(odd, 2 * plane + 2, CHUNKS - 2 * plane)
    held = jnp.where(odd, 2 * plane, jnp.maximum(CHUNKS - 2 - 2 * plane, 0))

    def hop(s, i, count):
        src = v_hbm.at[0:2, :, lanes(i)] if s == UP else v_hbm.at[rows - 2:rows, :, lanes(i)]
        slot = i - CHUNKS + count
        return pltpu.make_async_remote_copy(
            src_ref=src, dst_ref=hop_vm.at[slot], send_sem=row_send.at[s], recv_sem=hop_recv.at[slot],
            device_id=(gy + (2 if s == DOWN else -2), gx), device_id_type=MESH)

    def send_rows(i):
        for s in (UP, DOWN):
            detoured = crossing[s] & (i >= CHUNKS - late)
            when(exists(s) & jnp.logical_not(detoured), lambda s=s: row_copy(s, i).start())
            when(exists(s) & detoured, lambda s=s: hop(s, i, late).start())

    def hop_on(s, slot):
        i = CHUNKS - held + slot
        return pltpu.make_async_remote_copy(
            src_ref=hop_vm.at[slot], dst_ref=(down_vm if s == UP else up_vm).at[:, :, lanes(i)],
            send_sem=hop_send.at[slot], recv_sem=row_recv.at[s, i],
            device_id=(gy + (1 if s == UP else -1), gx), device_id_type=MESH)

    def each_held(slots, f):
        for s in (UP, DOWN):
            for slot in slots:
                when(crossing[s] & (slot < held), functools.partial(f, s, slot))

    def hop_pass(s, slot):
        hop(s, CHUNKS - held + slot, held).wait_recv()
        hop_on(s, slot).start()

    def col_copy(s, i):
        j = 2 - 2 * s
        return pltpu.make_async_remote_copy(
            src_ref=col_out.at[s, :, :, lanes(i)], dst_ref=col_vm.at[j:j + 2, 0:rows, lanes(i)],
            send_sem=col_send.at[s], recv_sem=col_recv.at[s, i // GROUP], device_id=at(LEFT + s), device_id_type=MESH)

    turns = ((gx == TURN + 1), (gx == TURN))

    def detour(s, i):
        first, second = RELAYS[1 - s]
        via = jnp.where(i % 3 == 0, first, second)
        return pltpu.make_async_remote_copy(
            src_ref=col_out.at[s, :, :, lanes(i)], dst_ref=relay_vm.at[i // 3],
            send_sem=col_send.at[s], recv_sem=relay_recv.at[i // 3], device_id=(gy, via), device_id_type=MESH)

    def send_cols(s, i):
        around = turns[s] & (i % 3 < 2)
        when(exists(LEFT + s) & jnp.logical_not(around), lambda: col_copy(s, i).start())
        when(around, lambda: detour(s, i).start())

    def forward(s, i):
        j = 2 - 2 * s
        return pltpu.make_async_remote_copy(
            src_ref=relay_vm.at[i // 3], dst_ref=col_vm.at[j:j + 2, 0:rows, lanes(i)],
            send_sem=relay_send.at[i // 3], recv_sem=col_recv.at[s, i // GROUP], device_id=(gy, TURN + s), device_id_type=MESH)

    def relays(f):
        for s in (0, 1):
            for n, via in enumerate(RELAYS[1 - s]):
                when(gx == via, functools.partial(f, s, n))

    def pass_on(j):
        def one(s, n):
            i = n + 3 * j
            if i < CHUNKS:
                detour(s, i).wait_recv()
                forward(s, i).start()
        relays(one)

    def passed_on(j):
        def one(s, n):
            i = n + 3 * j
            if i < CHUNKS:
                forward(s, i).wait_send()
        relays(one)

    def cor_copy(s, i):
        return pltpu.make_async_remote_copy(
            src_ref=corner_out.at[s, :, lanes(i)], dst_ref=corner_vm.at[s, :, lanes(i)],
            send_sem=cor_send.at[s], recv_sem=cor_recv.at[s, i], device_id=at(LEFT + s), device_id_type=MESH)

    def msg_copy(n):
        dy, dx = STEPS[n]
        src = row_msg.at[(dy + 1) // 2] if dy else col_msg.at[(dx + 1) // 2]
        return pltpu.make_async_remote_copy(
            src_ref=src, dst_ref=heard.at[n], send_sem=msg_send, recv_sem=msg_recv,
            device_id=at(n), device_id_type=MESH)

    def diag_copy(n):
        return pltpu.make_async_remote_copy(
            src_ref=diag_out.at[n - 4], dst_ref=diag_vm.at[n - 4], send_sem=diag_send.at[n - 4],
            recv_sem=diag_recv.at[n - 4], device_id=at(n), device_id_type=MESH)

    opposite = [STEPS.index((-dy, -dx)) for dy, dx in STEPS]

    def when(pred, f):
        pl.when(pred)(f)

    take_coef = pltpu.make_async_copy(coef_hbm, coef, coef_sem)
    barrier = pltpu.get_barrier_semaphore()
    take_coef.start()
    known = jnp.int32(0)
    for n in range(8):
        when(exists(n), lambda n=n: pl.semaphore_signal(barrier, inc=1, device_id=at(n), device_id_type=MESH))
        known = known + exists(n).astype(jnp.int32)
    for dy in (-2, 2):
        there = (gy + dy >= 0) & (gy + dy < ny)
        when(there, lambda dy=dy: pl.semaphore_signal(barrier, inc=1, device_id=(gy + dy, gx), device_id_type=MESH))
        known = known + there.astype(jnp.int32)
    for side in RELAYS:
        for via in side:
            for end in (TURN, TURN + 1):
                for me, other in ((via, end), (end, via)):
                    when(gx == me, lambda other=other: pl.semaphore_signal(barrier, inc=1, device_id=(gy, other), device_id_type=MESH))
                    known = known + (gx == me).astype(jnp.int32)
    padded[...] = jnp.zeros_like(padded)
    row_msg[...] = jnp.zeros_like(row_msg)
    col_msg[...] = jnp.zeros_like(col_msg)
    flipped[...] = jnp.zeros_like(flipped)
    take_coef.wait()
    for q in range(4):
        load(pl.ds(8 * q, 8)).start()
    padded[0:9, :, 0:cols] = coef[...]
    lane = lax.broadcasted_iota(jnp.int32, (8, 128), 1)
    for e, r in ((0, 0), (1, rows - 1)):
        for k in range(8):
            row_msg[e, k:k + 1, :] = padded[k, r:r + 1, :]
        last = pltpu.roll(jnp.broadcast_to(padded[8, r:r + 1, :], (8, 128)), 32, 1)
        row_msg[e] = jnp.where((lane >= 32) & (lane < 64), last, row_msg[e])
    for g in range(3):
        turned = padded[4 * g:4 * g + 4].reshape(128, 128).T
        col_msg[0, g:g + 1, :] = turned[0:1]
        col_msg[1, g:g + 1, :] = turned[cols - 1:cols]
        flipped[g, 1:cols + 1, :] = turned[0:cols]
    pl.semaphore_wait(barrier, known)

    for n in range(8):
        when(exists(n), lambda n=n: msg_copy(n).start())

    def rest(i, c):
        send_rows(i)
        return c

    lax.fori_loop(0, CHUNKS, rest, 0)

    def clear(ref):
        ref[...] = jnp.zeros_like(ref)

    when(jnp.logical_not(exists(UP)), lambda: clear(up_vm))
    when(jnp.logical_not(exists(DOWN)), lambda: clear(down_vm))
    for s in (0, 1):
        j = 2 - 2 * s
        when(jnp.logical_not(exists(LEFT + 1 - s)), lambda s=s, j=j: (clear(col_vm.at[j:j + 2]), clear(corner_vm.at[s]))[0])

    def pack(i, c):
        for s in (0, 1):
            for j in (0, 1):
                col = j if s == 0 else cols - 2 + j
                for r in range(0, rows, 8):
                    col_out[s, j, r:r + 8, lanes(i)] = v_vm[r:r + 8, col, lanes(i)]
        for s in (0, 1):
            send_cols(s, i)
        return c

    load(pl.ds(0, rows)).wait()
    lax.fori_loop(0, CHUNKS, pack, 0)
    for n in range(4, 8):
        dy, dx = STEPS[n]
        for c in (0, 1):
            for h in (0, 1):
                row, col = (h if dy < 0 else rows - 2 + h), (c if dx < 0 else cols - 2 + c)
                diag_out[n - 4, 2 * c + h:2 * c + h + 1, :] = v_vm[row, col:col + 1, lanes(CHUNKS - 1)]
        when(exists(n), lambda n=n: diag_copy(n).start())
        when(jnp.logical_not(exists(opposite[n])), lambda n=n: clear(diag_vm.at[n - 4]))

    def sent(ref, sem):
        pltpu.make_async_copy(ref, ref, sem).wait()

    neighbours = jnp.int32(0)
    for n in range(8):
        neighbours = neighbours + exists(n).astype(jnp.int32)

    def messages(sem):
        for n in (3, 5, 8):
            when(neighbours == n, lambda n=n: sent(heard.at[0:n], sem))

    messages(msg_recv)

    def from_side(n):
        return heard[opposite[n]]

    for g in range(3):
        flipped[g, 0:1, :] = jnp.where(exists(LEFT), from_side(LEFT)[g:g + 1], 0.0)
        flipped[g, cols + 1:cols + 2, :] = jnp.where(exists(RIGHT), from_side(RIGHT)[g:g + 1], 0.0)

    def rim(side, left, right):
        out = []
        for own, a, b in ((1, 97, 33), (97, 65, 1)):
            x = jnp.where(exists(side), pltpu.roll(from_side(side), own, 1), 0.0)
            x = jnp.where((lane == 0), jnp.where(exists(left), pltpu.roll(from_side(left), a, 1), 0.0), x)
            x = jnp.where((lane == cols + 1), jnp.where(exists(right), pltpu.roll(from_side(right), b, 1), 0.0), x)
            out.append(x)
        return out

    above = rim(UP, 4, 5)
    below = rim(DOWN, 6, 7)
    er = lax.broadcasted_iota(jnp.int32, (40, 128), 0)
    ec = lax.broadcasted_iota(jnp.int32, (40, 128), 1)
    row_at = gy * rows + er - 1
    col_at = gx * cols + ec - 1
    inside = (er < rows + 2) & (ec < cols + 2) & (row_at >= 0) & (row_at < rows_total) & (col_at >= 0) & (col_at < cols_total)
    for g in range(3):
        back = flipped[g].T
        for h in range(4):
            k = 4 * g + h
            if k < 9:
                a, b = k // 3 - 1, k % 3 - 1
                shifted[0, k, 1:rows + 1, :] = back[32 * h:32 * h + rows]
                which, line = (0, k) if k < 8 else (1, 0)
                shifted[0, k, 0:1, :] = above[which][line:line + 1]
                shifted[0, k, rows + 1:rows + 2, :] = below[which][line:line + 1]
                keep = inside & (row_at + a >= 0) & (row_at + a < rows_total) & (col_at + b >= 0) & (col_at + b < cols_total)
                x = jnp.where(keep, shifted[0, k], 0.0)
                shifted[0, k] = x
                shifted[1, k] = pltpu.roll(x, 127, 1)
                shifted[2, k] = pltpu.roll(x, 126, 1)
    terms = []
    for slot in range(25):
        total = None
        for at_pair in range(81):
            if SLOTS[at_pair] == slot:
                k, m = at_pair // 9, at_pair % 9
                a, b = k // 3 - 1, k % 3 - 1
                term = shifted[1 - b, k, 1 - a:1 - a + rows, :] * shifted[1 - b, m, 1 - a:1 - a + rows, :]
                total = term if total is None else total + term
        normal_ref[slot] = total[:, 0:cols]
        terms.append(total)
    for g in range(7):
        group = terms[4 * g:4 * g + 4]
        while len(group) < 4:
            group.append(jnp.zeros_like(group[0]))
        turned = jnp.concatenate(group, axis=0).T[0:cols]
        nts[0, g] = turned
        for b in range(1, 4):
            nts[b, g] = pltpu.roll(turned, 128 - 8 * b, 1)

    lane32 = lax.broadcasted_iota(jnp.int32, (cols, 128), 1)
    cell = lax.broadcasted_iota(jnp.int32, (cols, 128), 0)
    own_at, side_at = {}, {}
    for f in range(-2, 3):
        t = cell + f
        own_at[f] = jnp.where((t >= 0) & (t < cols), t, -1000)
        side_at[f] = jnp.where(t == -2, 0, jnp.where(t == -1, 32, jnp.where(t == cols, 64, jnp.where(t == cols + 1, 96, -1000))))

    def build(b, c):
        for rl in range(8):
            own = [jnp.zeros((cols, 128), F32) for _ in range(3)]
            side = jnp.zeros((cols, 128), F32)
            for e in range(-2, 3):
                spot = rl + e + 2
                tile, q = spot // 4, spot % 4
                row = b * 8 + rl + e
                slot = jnp.where(row < 0, 18 + row, row)
                slot = jnp.where(b == 3, jnp.where(row < rows, row - 16, row - 14), slot)
                for f in range(-2, 3):
                    index = (e + 2) * 5 + f + 2
                    at_lane = (index % 4) * 32 + rl
                    column = jnp.broadcast_to(nts[b, index // 4][:, at_lane:at_lane + 1], (cols, 128))
                    own[tile] = jnp.where(lane32 - 32 * q == own_at[f], column, own[tile])
                    if f:
                        side = jnp.where(lane32 - slot == side_at[f], column, side)
            for tile, x in enumerate(own + [side]):
                hi = x.astype(BF16)
                t_hi[b, rl * 32:rl * 32 + 32, tile * 128:tile * 128 + 128] = hi
                t_lo[b, rl * 32:rl * 32 + 32, tile * 128:tile * 128 + 128] = (x - hi.astype(F32)).astype(BF16)
        return c

    lax.fori_loop(0, 2, build, 0)
    pass_on(0)
    each_held((0, 1), hop_pass)
    lax.fori_loop(2, 4, build, 0)
    pass_on(1)
    each_held((2,), hop_pass)

    def halves(x):
        hi = x.astype(BF16)
        return hi, (x - hi.astype(F32)).astype(BF16)

    def put(i, block, start, hi, lo):
        w_hi[i % SETS, block, start:start + hi.shape[0], :] = hi
        w_lo[i % SETS, block, start:start + hi.shape[0], :] = lo

    def own_part(i):
        for q in range(4):
            hi, lo = halves(v_vm[8 * q:8 * q + 8, :, lanes(i)].reshape(256, width))
            put(i, q, 64, hi, lo)
            if q > 0:
                put(i, q - 1, 320, hi[0:64], lo[0:64])
            if q < 3:
                put(i, q + 1, 0, hi[192:256], lo[192:256])

    def side_part(i, last=False):
        def columns(s):
            j = 2 - 2 * s
            at_group = pl.ds(pl.multiple_of(i * width, width), GROUP * width)
            whole = col_vm.at[j:j + 2, 0:rows, at_group]
            pltpu.make_async_copy(whole, whole, col_recv.at[s, i // GROUP]).wait()

        for s in (0, 1):
            if not last:
                when(exists(LEFT + 1 - s) & (i % GROUP == 0), functools.partial(columns, s))
                when(exists(LEFT + 1 - s), lambda s=s: cor_copy(s, i).wait_recv())
        if last:
            for n in range(4, 8):
                when(exists(opposite[n]), lambda n=n: diag_copy(n).wait_recv())
        for j in range(4):
            hi, lo = halves(col_vm[j, 0:32, lanes(i)])
            if last:
                from_above, from_below = (6, 4) if j >= 2 else (7, 5)
                c = 2 * (j % 2)
                corner = jnp.concatenate([
                    diag_vm[from_above - 4, c:c + 2, :], diag_vm[from_below - 4, c:c + 2, :], jnp.zeros((12, width), F32)], axis=0)
            else:
                c = 4 * (j % 2)
                corner = jnp.concatenate([corner_vm[1 - j // 2, c:c + 4, lanes(i)], jnp.zeros((12, width), F32)], axis=0)
            chi, clo = halves(corner)
            put(i, 0, 384 + 32 * j, hi[0:16], lo[0:16])
            put(i, 0, 400 + 32 * j, chi, clo)
            put(i, 1, 384 + 32 * j, hi, lo)
            put(i, 2, 384 + 32 * j, hi, lo)
            put(i, 3, 384 + 32 * j, hi[16:32], lo[16:32])
            put(i, 3, 400 + 32 * j, chi, clo)

    def compute(i):
        side_part(i)
        for q in range(4):
            y = products(t_hi[q], t_lo[q], w_hi[i % SETS, q], w_lo[i % SETS, q])
            image_ref[8 * q:8 * q + 8, :, lanes(i)] = y.reshape(8, cols, width)

    def main(i, c):
        for step, slots in ((1, (3,)), (2, (4,)), (3, (5,))):
            when(i == step, lambda slots=slots: each_held(slots, hop_pass))
        when(i == 2, lambda: pass_on(2))
        own_part(i)
        when(i >= LAG, lambda: compute(i - LAG))
        for s in (UP, DOWN):
            when(exists(1 - s), lambda s=s: row_copy(s, i).wait_recv())
        for s in (0, 1):
            for j in (0, 1):
                col = j if s == 0 else cols - 2 + j
                for h in (0, 1):
                    corner_out[s, 4 * j + h:4 * j + h + 1, lanes(i)] = up_vm[h, col:col + 1, lanes(i)]
                    corner_out[s, 4 * j + 2 + h:4 * j + 3 + h, lanes(i)] = down_vm[h, col:col + 1, lanes(i)]
            when(exists(LEFT + s) & (i < CHUNKS - 1), lambda s=s: cor_copy(s, i).start())
        put(i, 0, 0, *halves(up_vm[:, :, lanes(i)].reshape(64, width)))
        put(i, 3, 320, *halves(down_vm[:, :, lanes(i)].reshape(64, width)))
        return c

    lax.fori_loop(0, CHUNKS, main, 0)
    for i in range(CHUNKS - LAG, CHUNKS - 1):
        side_part(i)
    side_part(CHUNKS - 1, last=True)

    for s in (0, 1):
        when(exists(s), lambda s=s: sent(up_vm, row_send.at[s]))
        when(exists(LEFT + s), lambda s=s: sent(col_out.at[s], col_send.at[s]))
        when(exists(LEFT + s), lambda s=s: sent(corner_out.at[s, :, span(CHUNKS - 1)], cor_send.at[s]))
    for n in range(4, 8):
        when(exists(n), lambda n=n: diag_copy(n).wait_send())
    messages(msg_send)
    for j in range(3):
        passed_on(j)
    each_held(range(6), lambda s, slot: hop_on(s, slot).wait_send())


def products(t_hi, t_lo, w_hi, w_lo):
    y = jnp.dot(t_hi, w_hi, preferred_element_type=F32)
    y = y + jnp.dot(t_lo, w_hi, preferred_element_type=F32)
    return y + jnp.dot(t_hi, w_lo, preferred_element_type=F32)


def last_chunks(normal_vm, image_vm, t_hi, t_lo, w_hi, w_lo, normal_hbm, image_hbm, tail, normal_sem, image_sem, tail_sem):
    rows, cols, nv = image_hbm.shape
    width = nv // CHUNKS
    done = nv - LAG * width
    copies = [pltpu.make_async_copy(
        image_vm.at[8 * q:8 * q + 8, :, :], image_hbm.at[8 * q:8 * q + 8, :, 0:done], image_sem.at[q]) for q in range(4)]
    copies.append(pltpu.make_async_copy(normal_vm, normal_hbm, normal_sem))
    for copy in copies:
        copy.start()
    for n in range(LAG):
        i = CHUNKS - LAG + n
        for q in range(4):
            y = products(t_hi[q], t_lo[q], w_hi[i % SETS, q], w_lo[i % SETS, q])
            tail[n, q] = y.reshape(8, cols, width)
            copies.append(pltpu.make_async_copy(
                tail.at[n, q], image_hbm.at[8 * q:8 * q + 8, :, i * width:i * width + width], tail_sem.at[n, q]))
            copies[-1].start()
    for copy in copies:
        copy.wait()


def per_device(rows_total, cols_total, coefficients, vectors):
    _, rows, cols = coefficients.shape
    nv = vectors.shape[2]
    width = nv // CHUNKS
    dma = pltpu.SemaphoreType.DMA
    parts = pl.pallas_call(
        functools.partial(kernel, rows_total, cols_total),
        out_shape=(
            pltpu.VMEM((25, rows, cols), F32), pltpu.VMEM((rows, cols, nv - LAG * width), F32),
            pltpu.VMEM((4, 256, 512), BF16), pltpu.VMEM((4, 256, 512), BF16),
            pltpu.VMEM((SETS, 4, 512, width), BF16), pltpu.VMEM((SETS, 4, 512, width), BF16)),
        in_specs=[pl.BlockSpec(memory_space=pltpu.HBM)] * 2,
        out_specs=(pl.BlockSpec(memory_space=pltpu.VMEM),) * 6,
        scratch_shapes=[
            pltpu.VMEM((9, rows, cols), F32),
            pltpu.VMEM((12, rows, 128), F32),
            pltpu.VMEM((3, 128, 128), F32),
            pltpu.VMEM((3, 9, 40, 128), F32),
            pltpu.VMEM((4, 7, cols, 128), F32),
            pltpu.VMEM((rows, cols, nv), F32),
            pltpu.VMEM((2, cols, nv), F32),
            pltpu.VMEM((2, cols, nv), F32),
            pltpu.VMEM((4, rows, nv), F32),
            pltpu.VMEM((2, 2, rows, nv), F32),
            pltpu.VMEM((2, 8, nv), F32),
            pltpu.VMEM((2, 8, nv), F32),
            pltpu.VMEM((3, 2, rows, width), F32),
            pltpu.VMEM((6, 2, cols, width), F32),
            pltpu.VMEM((4, 4, width), F32),
            pltpu.VMEM((4, 4, width), F32),
            pltpu.VMEM((2, 8, 128), F32),
            pltpu.VMEM((2, 8, 128), F32),
            pltpu.VMEM((8, 8, 128), F32),
            dma, dma,
            dma, dma,
            dma((2,)), dma((2, CHUNKS)),
            dma((2,)), dma((2, CHUNKS // GROUP)),
            dma((2,)), dma((2, CHUNKS - 1)),
            dma((3,)), dma((3,)),
            dma((6,)), dma((6,)),
            dma((4,)), dma((4,)),
        ],
        compiler_params=pltpu.CompilerParams(collective_id=0, has_side_effects=True, vmem_limit_bytes=44 * 2**20),
    )(pltpu.with_memory_space_constraint(coefficients, pltpu.HBM), vectors)
    return pl.pallas_call(
        last_chunks,
        out_shape=(jax.ShapeDtypeStruct((25, rows, cols), F32), jax.ShapeDtypeStruct((rows, cols, nv), F32)),
        in_specs=[pl.BlockSpec(memory_space=pltpu.VMEM)] * 6,
        out_specs=(pl.BlockSpec(memory_space=pltpu.HBM),) * 2,
        scratch_shapes=[pltpu.VMEM((LAG, 4, 8, cols, width), F32), dma, dma((4,)), dma((LAG, 4))],
        compiler_params=pltpu.CompilerParams(vmem_limit_bytes=8 * 2**20),
    )(*parts)


def solution(mesh):
    in_specs = (P(None, "gy", "gx"), P("gy", "gx", None))
    out_specs = (P(None, "gy", "gx"), P("gy", "gx", None))

    def whole(coefficients, vectors):
        body = functools.partial(per_device, coefficients.shape[1], coefficients.shape[2])
        return jax.shard_map(body, mesh=mesh, in_specs=in_specs, out_specs=out_specs, check_vma=False)(coefficients, vectors)

    return whole
```

```python
import functools

import jax
import jax.numpy as jnp
from jax import lax
from jax.experimental import pallas as pl
from jax.experimental.pallas import tpu as pltpu
from jax.sharding import PartitionSpec as P

MESH = pl.DeviceIdType.MESH
F32 = jnp.float32
BF16 = jnp.bfloat16
STEPS = ((-1, 0), (1, 0), (0, -1), (0, 1), (-1, -1), (-1, 1), (1, -1), (1, 1))
UP, DOWN, LEFT, RIGHT = 0, 1, 2, 3
CHUNKS = 8
GROUP = 4
LAG = 3
SETS = LAG + 1
NEAR = 2
SLOTS = [((m // 3 - k // 3) + 2) * 5 + (m % 3 - k % 3) + 2 for k in range(9) for m in range(9)]


RELAYS = (12, 11), (3, 4)
TURN = 7


def kernel(
    rows_total, cols_total,
    coef_hbm, v_hbm, normal_ref, image_ref, t_hi, t_lo, w_hi, w_lo,
    coef, padded, flipped, shifted, nts,
    v_vm, row_vm, col_vm, col_out, corner_out, corner_vm, relay_vm, hop_vm, diag_out, diag_vm,
    row_msg, col_msg, heard,
    load_sem, coef_sem, msg_send, msg_recv, row_send, row_recv, col_send, col_recv, cor_send, cor_recv,
    relay_recv, relay_send, hop_recv, hop_send, diag_send, diag_recv,
):
    gy = lax.axis_index("gy")
    gx = lax.axis_index("gx")
    ny = lax.axis_size("gy")
    nx = lax.axis_size("gx")
    rows, cols, nv = v_hbm.shape
    width = nv // CHUNKS

    def exists(n):
        dy, dx = STEPS[n]
        return (gy + dy >= 0) & (gy + dy < ny) & (gx + dx >= 0) & (gx + dx < nx)

    def at(n):
        dy, dx = STEPS[n]
        return (gy + dy, gx + dx)

    def lanes(i):
        return pl.ds(pl.multiple_of(i * width, width), width)

    up_vm, down_vm = row_vm.at[0], row_vm.at[1]

    def span(n):
        return pl.ds(0, n * width)

    def load(part):
        return pltpu.make_async_copy(v_hbm.at[part], v_vm.at[part], load_sem)

    def row_copy(s, i):
        src = v_hbm.at[0:2, :, lanes(i)] if s == UP else v_hbm.at[rows - 2:rows, :, lanes(i)]
        dst = down_vm if s == UP else up_vm
        return pltpu.make_async_remote_copy(
            src_ref=src, dst_ref=dst.at[:, :, lanes(i)], send_sem=row_send.at[s],
            recv_sem=row_recv.at[i], device_id=at(s), device_id_type=MESH)

    odd = gy % 2 == 1
    plane = gy // 2
    crossing = (jnp.logical_not(odd), odd)
    late = jnp.where(odd, 2 * plane + 2, CHUNKS - 2 * plane)
    relaying = jnp.where(odd, gy >= 2, gy < ny - 2)
    held = jnp.where(odd, 2 * plane, jnp.maximum(CHUNKS - 2 - 2 * plane, 0))

    def hop(s, i, count):
        src = v_hbm.at[0:2, :, lanes(i)] if s == UP else v_hbm.at[rows - 2:rows, :, lanes(i)]
        slot = i - CHUNKS + count
        return pltpu.make_async_remote_copy(
            src_ref=src, dst_ref=hop_vm.at[slot], send_sem=row_send.at[s], recv_sem=hop_recv.at[slot],
            device_id=(gy + (2 if s == DOWN else -2), gx), device_id_type=MESH)

    def send_rows(i):
        for s in (UP, DOWN):
            detoured = crossing[s] & (i >= CHUNKS - late)
            when(exists(s) & jnp.logical_not(detoured), lambda s=s: row_copy(s, i).start())
            when(exists(s) & detoured, lambda s=s: hop(s, i, late).start())

    def hop_on(s, slot):
        i = CHUNKS - held + slot
        return pltpu.make_async_remote_copy(
            src_ref=hop_vm.at[slot], dst_ref=(down_vm if s == UP else up_vm).at[:, :, lanes(i)],
            send_sem=hop_send, recv_sem=row_recv.at[i],
            device_id=(gy + (1 if s == UP else -1), gx), device_id_type=MESH)

    def each_held(slots, f):
        for s in (UP, DOWN):
            for slot in slots:
                when(crossing[s] & (slot < held), functools.partial(f, s, slot))

    def hop_pass(s, slot):
        hop(s, CHUNKS - held + slot, held).wait_recv()
        hop_on(s, slot).start()

    def col_copy(s, i):
        j = 2 - 2 * s
        return pltpu.make_async_remote_copy(
            src_ref=col_out.at[s, :, :, lanes(i)], dst_ref=col_vm.at[j:j + 2, 0:rows, lanes(i)],
            send_sem=col_send.at[s], recv_sem=col_recv.at[s, i // GROUP], device_id=at(LEFT + s), device_id_type=MESH)

    turns = ((gx == TURN + 1), (gx == TURN))

    def detour(s, i):
        first, second = RELAYS[1 - s]
        via = jnp.where(i % 3 == 0, first, second)
        return pltpu.make_async_remote_copy(
            src_ref=col_out.at[s, :, :, lanes(i)], dst_ref=relay_vm.at[i // 3],
            send_sem=col_send.at[s], recv_sem=relay_recv.at[i // 3], device_id=(gy, via), device_id_type=MESH)

    def send_cols(s, i):
        around = turns[s] & (i % 3 < 2)
        when(exists(LEFT + s) & jnp.logical_not(around), lambda: col_copy(s, i).start())
        when(around, lambda: detour(s, i).start())

    def forward(s, i):
        j = 2 - 2 * s
        return pltpu.make_async_remote_copy(
            src_ref=relay_vm.at[i // 3], dst_ref=col_vm.at[j:j + 2, 0:rows, lanes(i)],
            send_sem=relay_send, recv_sem=col_recv.at[s, i // GROUP], device_id=(gy, TURN + s), device_id_type=MESH)

    def relays(f):
        for s in (0, 1):
            for n, via in enumerate(RELAYS[1 - s]):
                when(gx == via, functools.partial(f, s, n))

    def pass_on(j):
        def one(s, n):
            i = n + 3 * j
            if i < CHUNKS:
                detour(s, i).wait_recv()
                forward(s, i).start()
        relays(one)

    def cor_copy(s, i):
        return pltpu.make_async_remote_copy(
            src_ref=corner_out.at[s, :, lanes(i)], dst_ref=corner_vm.at[s, :, lanes(i)],
            send_sem=cor_send.at[s], recv_sem=cor_recv.at[i], device_id=at(LEFT + s), device_id_type=MESH)

    def msg_copy(n):
        dy, dx = STEPS[n]
        src = row_msg.at[(dy + 1) // 2] if dy else col_msg.at[(dx + 1) // 2]
        return pltpu.make_async_remote_copy(
            src_ref=src, dst_ref=heard.at[n], send_sem=msg_send, recv_sem=msg_recv,
            device_id=at(n), device_id_type=MESH)

    def diag_copy(n):
        return pltpu.make_async_remote_copy(
            src_ref=diag_out.at[n - 4], dst_ref=diag_vm.at[n - 4], send_sem=diag_send,
            recv_sem=diag_recv, device_id=at(n), device_id_type=MESH)

    opposite = [STEPS.index((-dy, -dx)) for dy, dx in STEPS]

    def when(pred, f):
        pl.when(pred)(f)

    take_coef = pltpu.make_async_copy(coef_hbm, coef, coef_sem)
    barrier = pltpu.get_barrier_semaphore()
    take_coef.start()
    known = jnp.int32(0)
    for n in range(8):
        when(exists(n), lambda n=n: pl.semaphore_signal(barrier, inc=1, device_id=at(n), device_id_type=MESH))
        known = known + exists(n).astype(jnp.int32)
    for dy in (-2, 2):
        there = (gy + dy >= 0) & (gy + dy < ny)
        when(there, lambda dy=dy: pl.semaphore_signal(barrier, inc=1, device_id=(gy + dy, gx), device_id_type=MESH))
        known = known + there.astype(jnp.int32)
    for side in RELAYS:
        for via in side:
            for end in (TURN, TURN + 1):
                for me, other in ((via, end), (end, via)):
                    when(gx == me, lambda other=other: pl.semaphore_signal(barrier, inc=1, device_id=(gy, other), device_id_type=MESH))
                    known = known + (gx == me).astype(jnp.int32)
    padded[...] = jnp.zeros_like(padded)
    row_msg[...] = jnp.zeros_like(row_msg)
    col_msg[...] = jnp.zeros_like(col_msg)
    flipped[...] = jnp.zeros_like(flipped)
    take_coef.wait()
    for q in range(4):
        load(pl.ds(8 * q, 8)).start()
    padded[0:9, :, 0:cols] = coef[...]
    lane = lax.broadcasted_iota(jnp.int32, (8, 128), 1)
    for e, r in ((0, 0), (1, rows - 1)):
        for k in range(8):
            row_msg[e, k:k + 1, :] = padded[k, r:r + 1, :]
        last = pltpu.roll(jnp.broadcast_to(padded[8, r:r + 1, :], (8, 128)), 32, 1)
        row_msg[e] = jnp.where((lane >= 32) & (lane < 64), last, row_msg[e])
    for g in range(3):
        turned = padded[4 * g:4 * g + 4].reshape(128, 128).T
        col_msg[0, g:g + 1, :] = turned[0:1]
        col_msg[1, g:g + 1, :] = turned[cols - 1:cols]
        flipped[g, 1:cols + 1, :] = turned[0:cols]
    pl.semaphore_wait(barrier, known)

    for n in range(8):
        when(exists(n), lambda n=n: msg_copy(n).start())

    def rest(i, c):
        send_rows(i)
        return c

    lax.fori_loop(0, CHUNKS, rest, 0)

    def clear(ref):
        ref[...] = jnp.zeros_like(ref)

    when(jnp.logical_not(exists(UP)), lambda: clear(up_vm))
    when(jnp.logical_not(exists(DOWN)), lambda: clear(down_vm))
    for s in (0, 1):
        j = 2 - 2 * s
        when(jnp.logical_not(exists(LEFT + 1 - s)), lambda s=s, j=j: (clear(col_vm.at[j:j + 2]), clear(corner_vm.at[s]))[0])

    def pack(i, c):
        for s in (0, 1):
            for j in (0, 1):
                col = j if s == 0 else cols - 2 + j
                for r in range(0, rows, 8):
                    col_out[s, j, r:r + 8, lanes(i)] = v_vm[r:r + 8, col, lanes(i)]
        for s in (0, 1):
            send_cols(s, i)
        return c

    load(pl.ds(0, rows)).wait()
    lax.fori_loop(0, CHUNKS, pack, 0)
    for n in range(4, 8):
        dy, dx = STEPS[n]
        for c in (0, 1):
            for h in (0, 1):
                row, col = (h if dy < 0 else rows - 2 + h), (c if dx < 0 else cols - 2 + c)
                diag_out[n - 4, 2 * c + h:2 * c + h + 1, :] = v_vm[row, col:col + 1, nv - NEAR * width:nv]
        when(exists(n), lambda n=n: diag_copy(n).start())
        when(jnp.logical_not(exists(opposite[n])), lambda n=n: clear(diag_vm.at[n - 4]))

    def sent(ref, sem):
        pltpu.make_async_copy(ref, ref, sem).wait()

    neighbours = jnp.int32(0)
    for n in range(8):
        neighbours = neighbours + exists(n).astype(jnp.int32)

    def messages(sem):
        for n in (3, 5, 8):
            when(neighbours == n, lambda n=n: sent(heard.at[0:n], sem))

    corners = jnp.int32(0)
    for n in range(4, 8):
        corners = corners + exists(n).astype(jnp.int32)

    def diagonals(sem):
        for n in (1, 2, 4):
            when(corners == n, lambda n=n: sent(diag_vm.at[0:n], sem))

    def both_or_one(a, b, both, one, sem, i):
        pair = exists(a) & exists(b)
        when(pair, lambda: sent(both, sem.at[i]))
        when(jnp.logical_not(pair), lambda: sent(one, sem.at[i]))

    messages(msg_recv)

    def from_side(n):
        return heard[opposite[n]]

    for g in range(3):
        flipped[g, 0:1, :] = jnp.where(exists(LEFT), from_side(LEFT)[g:g + 1], 0.0)
        flipped[g, cols + 1:cols + 2, :] = jnp.where(exists(RIGHT), from_side(RIGHT)[g:g + 1], 0.0)

    def rim(side, left, right):
        out = []
        for own, a, b in ((1, 97, 33), (97, 65, 1)):
            x = jnp.where(exists(side), pltpu.roll(from_side(side), own, 1), 0.0)
            x = jnp.where((lane == 0), jnp.where(exists(left), pltpu.roll(from_side(left), a, 1), 0.0), x)
            x = jnp.where((lane == cols + 1), jnp.where(exists(right), pltpu.roll(from_side(right), b, 1), 0.0), x)
            out.append(x)
        return out

    above = rim(UP, 4, 5)
    below = rim(DOWN, 6, 7)
    er = lax.broadcasted_iota(jnp.int32, (40, 128), 0)
    ec = lax.broadcasted_iota(jnp.int32, (40, 128), 1)
    row_at = gy * rows + er - 1
    col_at = gx * cols + ec - 1
    inside = (er < rows + 2) & (ec < cols + 2) & (row_at >= 0) & (row_at < rows_total) & (col_at >= 0) & (col_at < cols_total)
    for g in range(3):
        back = flipped[g].T
        for h in range(4):
            k = 4 * g + h
            if k < 9:
                a, b = k // 3 - 1, k % 3 - 1
                shifted[0, k, 1:rows + 1, :] = back[32 * h:32 * h + rows]
                which, line = (0, k) if k < 8 else (1, 0)
                shifted[0, k, 0:1, :] = above[which][line:line + 1]
                shifted[0, k, rows + 1:rows + 2, :] = below[which][line:line + 1]
                keep = inside & (row_at + a >= 0) & (row_at + a < rows_total) & (col_at + b >= 0) & (col_at + b < cols_total)
                x = jnp.where(keep, shifted[0, k], 0.0)
                shifted[0, k] = x
                shifted[1, k] = pltpu.roll(x, 127, 1)
                shifted[2, k] = pltpu.roll(x, 126, 1)
    terms = []
    for slot in range(25):
        total = None
        for at_pair in range(81):
            if SLOTS[at_pair] == slot:
                k, m = at_pair // 9, at_pair % 9
                a, b = k // 3 - 1, k % 3 - 1
                term = shifted[1 - b, k, 1 - a:1 - a + rows, :] * shifted[1 - b, m, 1 - a:1 - a + rows, :]
                total = term if total is None else total + term
        normal_ref[slot] = total[:, 0:cols]
        terms.append(total)
    for g in range(7):
        group = terms[4 * g:4 * g + 4]
        while len(group) < 4:
            group.append(jnp.zeros_like(group[0]))
        turned = jnp.concatenate(group, axis=0).T[0:cols]
        nts[0, g] = turned
        for b in range(1, 4):
            nts[b, g] = pltpu.roll(turned, 128 - 8 * b, 1)

    lane32 = lax.broadcasted_iota(jnp.int32, (cols, 128), 1)
    cell = lax.broadcasted_iota(jnp.int32, (cols, 128), 0)
    own_at, side_at = {}, {}
    for f in range(-2, 3):
        t = cell + f
        own_at[f] = jnp.where((t >= 0) & (t < cols), t, -1000)
        side_at[f] = jnp.where(t == -2, 0, jnp.where(t == -1, 32, jnp.where(t == cols, 64, jnp.where(t == cols + 1, 96, -1000))))

    def build(b, c):
        for rl in range(8):
            own = [jnp.zeros((cols, 128), F32) for _ in range(3)]
            side = jnp.zeros((cols, 128), F32)
            for e in range(-2, 3):
                spot = rl + e + 2
                tile, q = spot // 4, spot % 4
                row = b * 8 + rl + e
                slot = jnp.where(row < 0, 18 + row, row)
                slot = jnp.where(b == 3, jnp.where(row < rows, row - 16, row - 14), slot)
                for f in range(-2, 3):
                    index = (e + 2) * 5 + f + 2
                    at_lane = (index % 4) * 32 + rl
                    column = jnp.broadcast_to(nts[b, index // 4][:, at_lane:at_lane + 1], (cols, 128))
                    own[tile] = jnp.where(lane32 - 32 * q == own_at[f], column, own[tile])
                    if f:
                        side = jnp.where(lane32 - slot == side_at[f], column, side)
            for tile, x in enumerate(own + [side]):
                hi = x.astype(BF16)
                t_hi[b, rl * 32:rl * 32 + 32, tile * 128:tile * 128 + 128] = hi
                t_lo[b, rl * 32:rl * 32 + 32, tile * 128:tile * 128 + 128] = (x - hi.astype(F32)).astype(BF16)
        return c

    lax.fori_loop(0, 2, build, 0)
    pass_on(0)
    each_held((0, 1), hop_pass)
    lax.fori_loop(2, 4, build, 0)
    pass_on(1)
    each_held((2,), hop_pass)

    def halves(x):
        hi = x.astype(BF16)
        return hi, (x - hi.astype(F32)).astype(BF16)

    def put(i, block, start, hi, lo):
        w_hi[i % SETS, block, start:start + hi.shape[0], :] = hi
        w_lo[i % SETS, block, start:start + hi.shape[0], :] = lo

    def own_part(i):
        for q in range(4):
            hi, lo = halves(v_vm[8 * q:8 * q + 8, :, lanes(i)].reshape(256, width))
            put(i, q, 64, hi, lo)
            if q > 0:
                put(i, q - 1, 320, hi[0:64], lo[0:64])
            if q < 3:
                put(i, q + 1, 0, hi[192:256], lo[192:256])

    def side_part(i, near=None):
        def columns(s):
            j = 2 - 2 * s
            at_group = pl.ds(pl.multiple_of(i * width, width), GROUP * width)
            whole = col_vm.at[j:j + 2, 0:rows, at_group]
            pltpu.make_async_copy(whole, whole, col_recv.at[s, i // GROUP]).wait()

        if near is None:
            for s in (0, 1):
                when(exists(LEFT + 1 - s) & (i % GROUP == 0), functools.partial(columns, s))
            both_or_one(LEFT, RIGHT, corner_vm.at[:, :, lanes(i)], corner_vm.at[0, :, lanes(i)], cor_recv, i)
        for j in range(4):
            hi, lo = halves(col_vm[j, 0:32, lanes(i)])
            if near is not None:
                at_near = slice(near * width, near * width + width)
                from_above, from_below = (6, 4) if j >= 2 else (7, 5)
                c = 2 * (j % 2)
                corner = jnp.concatenate([
                    diag_vm[from_above - 4, c:c + 2, at_near], diag_vm[from_below - 4, c:c + 2, at_near], jnp.zeros((12, width), F32)], axis=0)
            else:
                c = 4 * (j % 2)
                corner = jnp.concatenate([corner_vm[1 - j // 2, c:c + 4, lanes(i)], jnp.zeros((12, width), F32)], axis=0)
            chi, clo = halves(corner)
            put(i, 0, 384 + 32 * j, hi[0:16], lo[0:16])
            put(i, 0, 400 + 32 * j, chi, clo)
            put(i, 1, 384 + 32 * j, hi, lo)
            put(i, 2, 384 + 32 * j, hi, lo)
            put(i, 3, 384 + 32 * j, hi[16:32], lo[16:32])
            put(i, 3, 400 + 32 * j, chi, clo)

    def compute(i):
        side_part(i)
        for q in range(4):
            y = products(t_hi[q], t_lo[q], w_hi[i % SETS, q], w_lo[i % SETS, q])
            image_ref[8 * q:8 * q + 8, :, lanes(i)] = y.reshape(8, cols, width)

    def main(i, c):
        for step, slots in ((1, (3,)), (2, (4,)), (3, (5,))):
            when(i == step, lambda slots=slots: each_held(slots, hop_pass))
        when(i == 2, lambda: pass_on(2))
        own_part(i)
        when(i >= LAG, lambda: compute(i - LAG))
        both_or_one(UP, DOWN, row_vm.at[:, :, :, lanes(i)], up_vm.at[:, :, lanes(i)], row_recv, i)
        for s in (0, 1):
            for j in (0, 1):
                col = j if s == 0 else cols - 2 + j
                for h in (0, 1):
                    corner_out[s, 4 * j + h:4 * j + h + 1, lanes(i)] = up_vm[h, col:col + 1, lanes(i)]
                    corner_out[s, 4 * j + 2 + h:4 * j + 3 + h, lanes(i)] = down_vm[h, col:col + 1, lanes(i)]
            when(exists(LEFT + s) & (i < CHUNKS - NEAR), lambda s=s: cor_copy(s, i).start())
        put(i, 0, 0, *halves(up_vm[:, :, lanes(i)].reshape(64, width)))
        put(i, 3, 320, *halves(down_vm[:, :, lanes(i)].reshape(64, width)))
        return c

    lax.fori_loop(0, CHUNKS, main, 0)
    for i in range(CHUNKS - LAG, CHUNKS - NEAR):
        side_part(i)
    diagonals(diag_recv)
    for near in range(NEAR):
        side_part(CHUNKS - NEAR + near, near)

    for s in (0, 1):
        when(exists(s), lambda s=s: sent(up_vm, row_send.at[s]))
        when(exists(LEFT + s), lambda s=s: sent(col_out.at[s], col_send.at[s]))
        when(exists(LEFT + s), lambda s=s: sent(corner_out.at[s, :, span(CHUNKS - NEAR)], cor_send.at[s]))
    diagonals(diag_send)
    messages(msg_send)
    for side in RELAYS:
        for via in side:
            when(gx == via, lambda: sent(relay_vm, relay_send))
    for n in (2, 4, 6):
        when(relaying & (held == n), lambda n=n: sent(hop_vm.at[0:n], hop_send))


def products(t_hi, t_lo, w_hi, w_lo):
    y = jnp.dot(t_hi, w_hi, preferred_element_type=F32)
    y = y + jnp.dot(t_lo, w_hi, preferred_element_type=F32)
    return y + jnp.dot(t_hi, w_lo, preferred_element_type=F32)


def last_chunks(normal_vm, image_vm, t_hi, t_lo, w_hi, w_lo, normal_hbm, image_hbm, tail, normal_sem, image_sem, tail_sem):
    rows, cols, nv = image_hbm.shape
    width = nv // CHUNKS
    done = nv - LAG * width
    copies = [pltpu.make_async_copy(
        image_vm.at[8 * q:8 * q + 8, :, :], image_hbm.at[8 * q:8 * q + 8, :, 0:done], image_sem.at[q]) for q in range(4)]
    copies.append(pltpu.make_async_copy(normal_vm, normal_hbm, normal_sem))
    for copy in copies:
        copy.start()
    for n in range(LAG):
        i = CHUNKS - LAG + n
        for q in range(4):
            y = products(t_hi[q], t_lo[q], w_hi[i % SETS, q], w_lo[i % SETS, q])
            tail[n, q] = y.reshape(8, cols, width)
            copies.append(pltpu.make_async_copy(
                tail.at[n, q], image_hbm.at[8 * q:8 * q + 8, :, i * width:i * width + width], tail_sem.at[n, q]))
            copies[-1].start()
    for copy in copies:
        copy.wait()


def per_device(rows_total, cols_total, coefficients, vectors):
    _, rows, cols = coefficients.shape
    nv = vectors.shape[2]
    width = nv // CHUNKS
    dma = pltpu.SemaphoreType.DMA
    parts = pl.pallas_call(
        functools.partial(kernel, rows_total, cols_total),
        out_shape=(
            pltpu.VMEM((25, rows, cols), F32), pltpu.VMEM((rows, cols, nv - LAG * width), F32),
            pltpu.VMEM((4, 256, 512), BF16), pltpu.VMEM((4, 256, 512), BF16),
            pltpu.VMEM((SETS, 4, 512, width), BF16), pltpu.VMEM((SETS, 4, 512, width), BF16)),
        in_specs=[pl.BlockSpec(memory_space=pltpu.HBM)] * 2,
        out_specs=(pl.BlockSpec(memory_space=pltpu.VMEM),) * 6,
        scratch_shapes=[
            pltpu.VMEM((9, rows, cols), F32),
            pltpu.VMEM((12, rows, 128), F32),
            pltpu.VMEM((3, 128, 128), F32),
            pltpu.VMEM((3, 9, 40, 128), F32),
            pltpu.VMEM((4, 7, cols, 128), F32),
            pltpu.VMEM((rows, cols, nv), F32),
            pltpu.VMEM((2, 2, cols, nv), F32),
            pltpu.VMEM((4, rows, nv), F32),
            pltpu.VMEM((2, 2, rows, nv), F32),
            pltpu.VMEM((2, 8, nv), F32),
            pltpu.VMEM((2, 8, nv), F32),
            pltpu.VMEM((3, 2, rows, width), F32),
            pltpu.VMEM((6, 2, cols, width), F32),
            pltpu.VMEM((4, 4, NEAR * width), F32),
            pltpu.VMEM((4, 4, NEAR * width), F32),
            pltpu.VMEM((2, 8, 128), F32),
            pltpu.VMEM((2, 8, 128), F32),
            pltpu.VMEM((8, 8, 128), F32),
            dma, dma,
            dma, dma,
            dma((2,)), dma((CHUNKS,)),
            dma((2,)), dma((2, CHUNKS // GROUP)),
            dma((2,)), dma((CHUNKS - NEAR,)),
            dma((3,)), dma,
            dma((6,)), dma,
            dma, dma,
        ],
        compiler_params=pltpu.CompilerParams(collective_id=0, has_side_effects=True, vmem_limit_bytes=44 * 2**20),
    )(pltpu.with_memory_space_constraint(coefficients, pltpu.HBM), vectors)
    return pl.pallas_call(
        last_chunks,
        out_shape=(jax.ShapeDtypeStruct((25, rows, cols), F32), jax.ShapeDtypeStruct((rows, cols, nv), F32)),
        in_specs=[pl.BlockSpec(memory_space=pltpu.VMEM)] * 6,
        out_specs=(pl.BlockSpec(memory_space=pltpu.HBM),) * 2,
        scratch_shapes=[pltpu.VMEM((LAG, 4, 8, cols, width), F32), dma, dma((4,)), dma((LAG, 4))],
        compiler_params=pltpu.CompilerParams(vmem_limit_bytes=8 * 2**20),
    )(*parts)


def solution(mesh):
    in_specs = (P(None, "gy", "gx"), P("gy", "gx", None))
    out_specs = (P(None, "gy", "gx"), P("gy", "gx", None))

    def whole(coefficients, vectors):
        body = functools.partial(per_device, coefficients.shape[1], coefficients.shape[2])
        return jax.shard_map(body, mesh=mesh, in_specs=in_specs, out_specs=out_specs, check_vma=False)(coefficients, vectors)

    return whole
```

```python
import functools

import jax
import jax.numpy as jnp
from jax import lax
from jax.experimental import pallas as pl
from jax.experimental.pallas import tpu as pltpu
from jax.sharding import PartitionSpec as P

MESH = pl.DeviceIdType.MESH
F32 = jnp.float32
BF16 = jnp.bfloat16
STEPS = ((-1, 0), (1, 0), (0, -1), (0, 1), (-1, -1), (-1, 1), (1, -1), (1, 1))
UP, DOWN, LEFT, RIGHT = 0, 1, 2, 3
CHUNKS = 8
GROUP = 4
LAG = 3
SETS = LAG + 1
NEAR = 2
SLOTS = [((m // 3 - k // 3) + 2) * 5 + (m % 3 - k % 3) + 2 for k in range(9) for m in range(9)]


RELAYS = (12, 11, 15), (3, 4, 0)
TURN = 7


def kernel(
    rows_total, cols_total,
    coef_hbm, v_hbm, normal_ref, image_ref, t_hi, t_lo, w_hi, w_lo,
    coef, padded, flipped, shifted, nts,
    v_vm, row_vm, col_vm, col_out, corner_out, corner_vm, relay_vm, hop_vm, diag_out, diag_vm,
    row_msg, col_msg, heard,
    load_sem, edge_sem, ready_sem, coef_sem, msg_send, msg_recv, row_send, row_recv, col_send, col_recv, cor_send, cor_recv,
    relay_recv, relay_send, hop_recv, hop_send, diag_send, diag_recv,
):
    gy = lax.axis_index("gy")
    gx = lax.axis_index("gx")
    ny = lax.axis_size("gy")
    nx = lax.axis_size("gx")
    rows, cols, nv = v_hbm.shape
    width = nv // CHUNKS

    def exists(n):
        dy, dx = STEPS[n]
        return (gy + dy >= 0) & (gy + dy < ny) & (gx + dx >= 0) & (gx + dx < nx)

    def at(n):
        dy, dx = STEPS[n]
        return (gy + dy, gx + dx)

    def lanes(i):
        return pl.ds(pl.multiple_of(i * width, width), width)

    up_vm, down_vm = row_vm.at[0], row_vm.at[1]

    def span(n):
        return pl.ds(0, n * width)

    def load(first, count, sem):
        part = pl.ds(first, count)
        return pltpu.make_async_copy(v_hbm.at[part], v_vm.at[part], sem)

    def row_copy(s, i):
        src = v_vm.at[0:2, :, lanes(i)] if s == UP else v_vm.at[rows - 2:rows, :, lanes(i)]
        dst = down_vm if s == UP else up_vm
        return pltpu.make_async_remote_copy(
            src_ref=src, dst_ref=dst.at[:, :, lanes(i)], send_sem=row_send.at[s],
            recv_sem=row_recv.at[i], device_id=at(s), device_id_type=MESH)

    odd = gy % 2 == 1
    plane = gy // 2
    crossing = (jnp.logical_not(odd), odd)
    late = jnp.where(odd, 2 * plane + 2, CHUNKS - 2 * plane)
    relaying = jnp.where(odd, gy >= 2, gy < ny - 2)
    held = jnp.where(odd, 2 * plane, jnp.maximum(CHUNKS - 2 - 2 * plane, 0))

    def hop(s, i, count):
        src = v_vm.at[0:2, :, lanes(i)] if s == UP else v_vm.at[rows - 2:rows, :, lanes(i)]
        slot = i - CHUNKS + count
        return pltpu.make_async_remote_copy(
            src_ref=src, dst_ref=hop_vm.at[slot], send_sem=row_send.at[s], recv_sem=hop_recv.at[slot],
            device_id=(gy + (2 if s == DOWN else -2), gx), device_id_type=MESH)

    def send_rows(i):
        for s in (UP, DOWN):
            detoured = crossing[s] & (i >= CHUNKS - late)
            when(exists(s) & jnp.logical_not(detoured), lambda s=s: row_copy(s, i).start())

    def send_hops(i):
        for s in (UP, DOWN):
            when(exists(s) & crossing[s] & (i >= CHUNKS - late), lambda s=s: hop(s, i, late).start())

    def hop_on(s, slot):
        i = CHUNKS - held + slot
        return pltpu.make_async_remote_copy(
            src_ref=hop_vm.at[slot], dst_ref=(down_vm if s == UP else up_vm).at[:, :, lanes(i)],
            send_sem=hop_send, recv_sem=row_recv.at[i],
            device_id=(gy + (1 if s == UP else -1), gx), device_id_type=MESH)

    def each_held(slots, f, only=True):
        for s in (UP, DOWN):
            for slot in slots:
                when(crossing[s] & (slot < held) & only, functools.partial(f, s, slot))

    def hop_pass(s, slot):
        hop(s, CHUNKS - held + slot, held).wait_recv()
        hop_on(s, slot).start()

    def col_copy(s, i):
        j = 2 - 2 * s
        return pltpu.make_async_remote_copy(
            src_ref=col_out.at[s, :, :, lanes(i)], dst_ref=col_vm.at[j:j + 2, 0:rows, lanes(i)],
            send_sem=col_send.at[s], recv_sem=col_recv.at[s, i // GROUP], device_id=at(LEFT + s), device_id_type=MESH)

    turns = ((gx == TURN + 1), (gx == TURN))

    def detour(s, i, n):
        slot = jnp.where(n == 2, i - 6, i // 3)
        first, second, third = RELAYS[1 - s]
        via = jnp.where(n == 2, third, jnp.where(n == 0, first, second))
        return pltpu.make_async_remote_copy(
            src_ref=col_out.at[s, :, :, lanes(i)], dst_ref=relay_vm.at[slot],
            send_sem=col_send.at[s], recv_sem=relay_recv.at[slot], device_id=(gy, via), device_id_type=MESH)

    def send_cols(s, i):
        around = turns[s] & ((i % 3 < 2) | (i >= 6))
        when(exists(LEFT + s) & jnp.logical_not(around), lambda: col_copy(s, i).start())
        when(around, lambda: detour(s, i, jnp.where(i >= 6, 2, i % 3)).start())

    def pass_on(slot, late):
        for s in (0, 1):
            for n, via in enumerate(RELAYS[1 - s]):
                if late == (n == 2):
                    i = 6 + slot if late else n + 3 * slot

                    def one(s=s, n=n, i=i):
                        detour(s, i, n).wait_recv()
                        j = 2 - 2 * s
                        pltpu.make_async_remote_copy(
                            src_ref=relay_vm.at[slot], dst_ref=col_vm.at[j:j + 2, 0:rows, lanes(i)], send_sem=relay_send,
                            recv_sem=col_recv.at[s, i // GROUP], device_id=(gy, TURN + s), device_id_type=MESH).start()

                    when(gx == via, one)

    def cor_copy(s, i):
        return pltpu.make_async_remote_copy(
            src_ref=corner_out.at[s, :, lanes(i)], dst_ref=corner_vm.at[s, :, lanes(i)],
            send_sem=cor_send.at[s], recv_sem=cor_recv.at[i], device_id=at(LEFT + s), device_id_type=MESH)

    def msg_copy(n):
        dy, dx = STEPS[n]
        src = row_msg.at[(dy + 1) // 2] if dy else col_msg.at[(dx + 1) // 2]
        return pltpu.make_async_remote_copy(
            src_ref=src, dst_ref=heard.at[n], send_sem=msg_send, recv_sem=msg_recv,
            device_id=at(n), device_id_type=MESH)

    def diag_copy(n):
        return pltpu.make_async_remote_copy(
            src_ref=diag_out.at[n - 4], dst_ref=diag_vm.at[n - 4], send_sem=diag_send,
            recv_sem=diag_recv, device_id=at(n), device_id_type=MESH)

    opposite = [STEPS.index((-dy, -dx)) for dy, dx in STEPS]

    def when(pred, f):
        pl.when(pred)(f)

    take_coef = pltpu.make_async_copy(coef_hbm, coef, coef_sem)
    barrier = pltpu.get_barrier_semaphore()
    take_coef.start()
    load(0, 2, edge_sem.at[0]).start()
    load(rows - 2, 2, edge_sem.at[1]).start()
    known = jnp.int32(0)
    for n in range(4):
        when(exists(n), lambda n=n: pl.semaphore_signal(barrier, inc=1, device_id=at(n), device_id_type=MESH))
        known = known + exists(n).astype(jnp.int32)
    for dy in (-2, 2):
        there = (gy + dy >= 0) & (gy + dy < ny)
        when(there, lambda dy=dy: pl.semaphore_signal(barrier, inc=1, device_id=(gy + dy, gx), device_id_type=MESH))
        known = known + there.astype(jnp.int32)
    for side in RELAYS:
        for via in side:
            for end in (TURN, TURN + 1):
                for me, other in ((via, end), (end, via)):
                    when(gx == me, lambda other=other: pl.semaphore_signal(barrier, inc=1, device_id=(gy, other), device_id_type=MESH))
                    known = known + (gx == me).astype(jnp.int32)
    padded[...] = jnp.zeros_like(padded)
    row_msg[...] = jnp.zeros_like(row_msg)
    col_msg[...] = jnp.zeros_like(col_msg)
    flipped[...] = jnp.zeros_like(flipped)
    take_coef.wait()
    load(2, rows - 4, load_sem).start()
    padded[0:9, :, 0:cols] = coef[...]
    lane = lax.broadcasted_iota(jnp.int32, (8, 128), 1)
    for e, r in ((0, 0), (1, rows - 1)):
        for k in range(8):
            row_msg[e, k:k + 1, :] = padded[k, r:r + 1, :]
        last = pltpu.roll(jnp.broadcast_to(padded[8, r:r + 1, :], (8, 128)), 32, 1)
        row_msg[e] = jnp.where((lane >= 32) & (lane < 64), last, row_msg[e])
    for g in range(3):
        turned = padded[4 * g:4 * g + 4].reshape(128, 128).T
        col_msg[0, g:g + 1, :] = turned[0:1]
        col_msg[1, g:g + 1, :] = turned[cols - 1:cols]
        flipped[g, 1:cols + 1, :] = turned[0:cols]
    load(0, 2, edge_sem.at[0]).wait()
    load(rows - 2, 2, edge_sem.at[1]).wait()
    pl.semaphore_wait(barrier, known)

    for n in (LEFT, RIGHT):
        when(exists(n), lambda n=n: pl.semaphore_signal(ready_sem, inc=1, device_id=at(n), device_id_type=MESH))
    for n in range(4):
        when(exists(n), lambda n=n: msg_copy(n).start())
    send_rows(0)
    pl.semaphore_wait(ready_sem, exists(LEFT).astype(jnp.int32) + exists(RIGHT).astype(jnp.int32))
    for n in range(4, 8):
        when(exists(n), lambda n=n: msg_copy(n).start())

    def rest(i, c):
        send_rows(i)
        return c

    def hops(i, c):
        send_hops(i)
        return c

    lax.fori_loop(2, CHUNKS, hops, 0)

    lax.fori_loop(1, CHUNKS - 3, rest, 0)

    def clear(ref):
        ref[...] = jnp.zeros_like(ref)

    when(jnp.logical_not(exists(UP)), lambda: clear(up_vm))
    when(jnp.logical_not(exists(DOWN)), lambda: clear(down_vm))
    for s in (0, 1):
        j = 2 - 2 * s
        when(jnp.logical_not(exists(LEFT + 1 - s)), lambda s=s, j=j: (clear(col_vm.at[j:j + 2]), clear(corner_vm.at[s]))[0])

    def pack(i, c):
        for s in (0, 1):
            for j in (0, 1):
                col = j if s == 0 else cols - 2 + j
                for r in range(0, rows, 8):
                    col_out[s, j, r:r + 8, lanes(i)] = v_vm[r:r + 8, col, lanes(i)]
        for s in (0, 1):
            send_cols(s, i)
        return c

    load(2, rows - 4, load_sem).wait()
    lax.fori_loop(0, CHUNKS, pack, 0)
    for n in range(4, 8):
        dy, dx = STEPS[n]
        for c in (0, 1):
            for h in (0, 1):
                row, col = (h if dy < 0 else rows - 2 + h), (c if dx < 0 else cols - 2 + c)
                diag_out[n - 4, 2 * c + h:2 * c + h + 1, :] = v_vm[row, col:col + 1, nv - NEAR * width:nv]
        when(exists(n), lambda n=n: diag_copy(n).start())
        when(jnp.logical_not(exists(opposite[n])), lambda n=n: clear(diag_vm.at[n - 4]))

    def sent(ref, sem):
        pltpu.make_async_copy(ref, ref, sem).wait()

    neighbours = jnp.int32(0)
    for n in range(8):
        neighbours = neighbours + exists(n).astype(jnp.int32)

    def messages(sem):
        for n in (3, 5, 8):
            when(neighbours == n, lambda n=n: sent(heard.at[0:n], sem))

    corners = jnp.int32(0)
    for n in range(4, 8):
        corners = corners + exists(n).astype(jnp.int32)

    def diagonals(sem):
        for n in (1, 2, 4):
            when(corners == n, lambda n=n: sent(diag_vm.at[0:n], sem))

    def both_or_one(a, b, both, one, sem, i):
        pair = exists(a) & exists(b)
        when(pair, lambda: sent(both, sem.at[i]))
        when(jnp.logical_not(pair), lambda: sent(one, sem.at[i]))

    messages(msg_recv)

    def from_side(n):
        return heard[opposite[n]]

    for g in range(3):
        flipped[g, 0:1, :] = jnp.where(exists(LEFT), from_side(LEFT)[g:g + 1], 0.0)
        flipped[g, cols + 1:cols + 2, :] = jnp.where(exists(RIGHT), from_side(RIGHT)[g:g + 1], 0.0)

    def rim(side, left, right):
        out = []
        for own, a, b in ((1, 97, 33), (97, 65, 1)):
            x = jnp.where(exists(side), pltpu.roll(from_side(side), own, 1), 0.0)
            x = jnp.where((lane == 0), jnp.where(exists(left), pltpu.roll(from_side(left), a, 1), 0.0), x)
            x = jnp.where((lane == cols + 1), jnp.where(exists(right), pltpu.roll(from_side(right), b, 1), 0.0), x)
            out.append(x)
        return out

    above = rim(UP, 4, 5)
    below = rim(DOWN, 6, 7)
    er = lax.broadcasted_iota(jnp.int32, (40, 128), 0)
    ec = lax.broadcasted_iota(jnp.int32, (40, 128), 1)
    row_at = gy * rows + er - 1
    col_at = gx * cols + ec - 1
    inside = (er < rows + 2) & (ec < cols + 2) & (row_at >= 0) & (row_at < rows_total) & (col_at >= 0) & (col_at < cols_total)
    for g in range(3):
        back = flipped[g].T
        for h in range(4):
            k = 4 * g + h
            if k < 9:
                a, b = k // 3 - 1, k % 3 - 1
                shifted[0, k, 1:rows + 1, :] = back[32 * h:32 * h + rows]
                which, line = (0, k) if k < 8 else (1, 0)
                shifted[0, k, 0:1, :] = above[which][line:line + 1]
                shifted[0, k, rows + 1:rows + 2, :] = below[which][line:line + 1]
                keep = inside & (row_at + a >= 0) & (row_at + a < rows_total) & (col_at + b >= 0) & (col_at + b < cols_total)
                x = jnp.where(keep, shifted[0, k], 0.0)
                shifted[0, k] = x
                shifted[1, k] = pltpu.roll(x, 127, 1)
                shifted[2, k] = pltpu.roll(x, 126, 1)
    terms = []
    for slot in range(25):
        total = None
        for at_pair in range(81):
            if SLOTS[at_pair] == slot:
                k, m = at_pair // 9, at_pair % 9
                a, b = k // 3 - 1, k % 3 - 1
                term = shifted[1 - b, k, 1 - a:1 - a + rows, :] * shifted[1 - b, m, 1 - a:1 - a + rows, :]
                total = term if total is None else total + term
        normal_ref[slot] = total[:, 0:cols]
        terms.append(total)
    for g in range(7):
        group = terms[4 * g:4 * g + 4]
        while len(group) < 4:
            group.append(jnp.zeros_like(group[0]))
        turned = jnp.concatenate(group, axis=0).T[0:cols]
        nts[0, g] = turned
        for b in range(1, 4):
            nts[b, g] = pltpu.roll(turned, 128 - 8 * b, 1)

    lane32 = lax.broadcasted_iota(jnp.int32, (cols, 128), 1)
    cell = lax.broadcasted_iota(jnp.int32, (cols, 128), 0)
    own_at, side_at = {}, {}
    for f in range(-2, 3):
        t = cell + f
        own_at[f] = jnp.where((t >= 0) & (t < cols), t, -1000)
        side_at[f] = jnp.where(t == -2, 0, jnp.where(t == -1, 32, jnp.where(t == cols, 64, jnp.where(t == cols + 1, 96, -1000))))

    def build(b, c):
        for rl in range(8):
            own = [jnp.zeros((cols, 128), F32) for _ in range(3)]
            side = jnp.zeros((cols, 128), F32)
            for e in range(-2, 3):
                spot = rl + e + 2
                tile, q = spot // 4, spot % 4
                row = b * 8 + rl + e
                slot = jnp.where(row < 0, 18 + row, row)
                slot = jnp.where(b == 3, jnp.where(row < rows, row - 16, row - 14), slot)
                for f in range(-2, 3):
                    index = (e + 2) * 5 + f + 2
                    at_lane = (index % 4) * 32 + rl
                    column = jnp.broadcast_to(nts[b, index // 4][:, at_lane:at_lane + 1], (cols, 128))
                    own[tile] = jnp.where(lane32 - 32 * q == own_at[f], column, own[tile])
                    if f:
                        side = jnp.where(lane32 - slot == side_at[f], column, side)
            for tile, x in enumerate(own + [side]):
                hi = x.astype(BF16)
                t_hi[b, rl * 32:rl * 32 + 32, tile * 128:tile * 128 + 128] = hi
                t_lo[b, rl * 32:rl * 32 + 32, tile * 128:tile * 128 + 128] = (x - hi.astype(F32)).astype(BF16)
        return c

    each_held((0, 1), hop_pass, held > 2)
    send_rows(CHUNKS - 3)
    lax.fori_loop(0, 2, build, 0)
    pass_on(0, False)
    each_held((2,), hop_pass)
    send_rows(CHUNKS - 2)
    lax.fori_loop(2, 4, build, 0)
    pass_on(1, False)
    each_held((3,), hop_pass)
    each_held((0, 1), hop_pass, held == 2)
    send_rows(CHUNKS - 1)

    def halves(x):
        hi = x.astype(BF16)
        return hi, (x - hi.astype(F32)).astype(BF16)

    def put(i, block, start, hi, lo):
        w_hi[i % SETS, block, start:start + hi.shape[0], :] = hi
        w_lo[i % SETS, block, start:start + hi.shape[0], :] = lo

    def own_part(i):
        for q in range(4):
            hi, lo = halves(v_vm[8 * q:8 * q + 8, :, lanes(i)].reshape(256, width))
            put(i, q, 64, hi, lo)
            if q > 0:
                put(i, q - 1, 320, hi[0:64], lo[0:64])
            if q < 3:
                put(i, q + 1, 0, hi[192:256], lo[192:256])

    def side_part(i, near=None):
        def columns(s):
            j = 2 - 2 * s
            at_group = pl.ds(pl.multiple_of(i * width, width), GROUP * width)
            whole = col_vm.at[j:j + 2, 0:rows, at_group]
            pltpu.make_async_copy(whole, whole, col_recv.at[s, i // GROUP]).wait()

        if near is None:
            for s in (0, 1):
                when(exists(LEFT + 1 - s) & (i % GROUP == 0), functools.partial(columns, s))
            both_or_one(LEFT, RIGHT, corner_vm.at[:, :, lanes(i)], corner_vm.at[0, :, lanes(i)], cor_recv, i)
        for j in range(4):
            hi, lo = halves(col_vm[j, 0:32, lanes(i)])
            if near is not None:
                at_near = slice(near * width, near * width + width)
                from_above, from_below = (6, 4) if j >= 2 else (7, 5)
                c = 2 * (j % 2)
                corner = jnp.concatenate([
                    diag_vm[from_above - 4, c:c + 2, at_near], diag_vm[from_below - 4, c:c + 2, at_near], jnp.zeros((12, width), F32)], axis=0)
            else:
                c = 4 * (j % 2)
                corner = jnp.concatenate([corner_vm[1 - j // 2, c:c + 4, lanes(i)], jnp.zeros((12, width), F32)], axis=0)
            chi, clo = halves(corner)
            put(i, 0, 384 + 32 * j, hi[0:16], lo[0:16])
            put(i, 0, 400 + 32 * j, chi, clo)
            put(i, 1, 384 + 32 * j, hi, lo)
            put(i, 2, 384 + 32 * j, hi, lo)
            put(i, 3, 384 + 32 * j, hi[16:32], lo[16:32])
            put(i, 3, 400 + 32 * j, chi, clo)

    def compute(i):
        side_part(i)
        for q in range(4):
            y = products(t_hi[q], t_lo[q], w_hi[i % SETS, q], w_lo[i % SETS, q])
            image_ref[8 * q:8 * q + 8, :, lanes(i)] = y.reshape(8, cols, width)

    turned = turns[0] | turns[1]

    def computed(i):
        late_count = jnp.clip(i - 2, 0, CHUNKS - LAG)
        return jnp.where(turned | (i < CHUNKS - 3), late_count, jnp.minimum(i - 1, CHUNKS - LAG))

    def main(i, c):
        for step, slots in ((1, (4,)), (2, (5,))):
            when(i == step, lambda slots=slots: each_held(slots, hop_pass))
        for step in (3, 4):
            when(i == step, functools.partial(pass_on, step - 3, True))
        own_part(i)
        lax.fori_loop(computed(i - 1), computed(i), lambda c, x: (compute(c), x)[1], 0)
        both_or_one(UP, DOWN, row_vm.at[:, :, :, lanes(i)], up_vm.at[:, :, lanes(i)], row_recv, i)
        for s in (0, 1):
            for j in (0, 1):
                col = j if s == 0 else cols - 2 + j
                for h in (0, 1):
                    corner_out[s, 4 * j + h:4 * j + h + 1, lanes(i)] = up_vm[h, col:col + 1, lanes(i)]
                    corner_out[s, 4 * j + 2 + h:4 * j + 3 + h, lanes(i)] = down_vm[h, col:col + 1, lanes(i)]
            when(exists(LEFT + s) & (i < CHUNKS - NEAR), lambda s=s: cor_copy(s, i).start())
        put(i, 0, 0, *halves(up_vm[:, :, lanes(i)].reshape(64, width)))
        put(i, 3, 320, *halves(down_vm[:, :, lanes(i)].reshape(64, width)))
        return c

    lax.fori_loop(0, CHUNKS, main, 0)
    for i in range(CHUNKS - LAG, CHUNKS - NEAR):
        side_part(i)
    diagonals(diag_recv)
    for near in range(NEAR):
        side_part(CHUNKS - NEAR + near, near)

    for s in (0, 1):
        when(exists(s), lambda s=s: sent(up_vm, row_send.at[s]))
        when(exists(LEFT + s), lambda s=s: sent(col_out.at[s], col_send.at[s]))
        when(exists(LEFT + s), lambda s=s: sent(corner_out.at[s, :, span(CHUNKS - NEAR)], cor_send.at[s]))
    diagonals(diag_send)
    messages(msg_send)
    for side in RELAYS:
        for via in side:
            when(gx == via, lambda: sent(relay_vm, relay_send))
    for n in (2, 4, 6):
        when(relaying & (held == n), lambda n=n: sent(hop_vm.at[0:n], hop_send))


def products(t_hi, t_lo, w_hi, w_lo):
    y = jnp.dot(t_hi, w_hi, preferred_element_type=F32)
    y = y + jnp.dot(t_lo, w_hi, preferred_element_type=F32)
    return y + jnp.dot(t_hi, w_lo, preferred_element_type=F32)


def last_chunks(normal_vm, image_vm, t_hi, t_lo, w_hi, w_lo, normal_hbm, image_hbm, tail, normal_sem, image_sem):
    rows, cols, nv = image_hbm.shape
    width = nv // CHUNKS
    done = nv - LAG * width
    for q in range(4):
        pltpu.make_async_copy(
            image_vm.at[8 * q:8 * q + 8, :, :], image_hbm.at[8 * q:8 * q + 8, :, 0:done], image_sem).start()
    write_normal = pltpu.make_async_copy(normal_vm, normal_hbm, normal_sem)
    write_normal.start()
    for n in range(LAG):
        i = CHUNKS - LAG + n
        for q in range(4):
            y = products(t_hi[q], t_lo[q], w_hi[i % SETS, q], w_lo[i % SETS, q])
            tail[n, q] = y.reshape(8, cols, width)
            pltpu.make_async_copy(
                tail.at[n, q], image_hbm.at[8 * q:8 * q + 8, :, i * width:i * width + width], image_sem).start()
    pltpu.make_async_copy(image_hbm, image_hbm, image_sem).wait()
    write_normal.wait()


def per_device(rows_total, cols_total, coefficients, vectors):
    _, rows, cols = coefficients.shape
    nv = vectors.shape[2]
    width = nv // CHUNKS
    dma = pltpu.SemaphoreType.DMA
    parts = pl.pallas_call(
        functools.partial(kernel, rows_total, cols_total),
        out_shape=(
            pltpu.VMEM((25, rows, cols), F32), pltpu.VMEM((rows, cols, nv - LAG * width), F32),
            pltpu.VMEM((4, 256, 512), BF16), pltpu.VMEM((4, 256, 512), BF16),
            pltpu.VMEM((SETS, 4, 512, width), BF16), pltpu.VMEM((SETS, 4, 512, width), BF16)),
        in_specs=[pl.BlockSpec(memory_space=pltpu.HBM)] * 2,
        out_specs=(pl.BlockSpec(memory_space=pltpu.VMEM),) * 6,
        scratch_shapes=[
            pltpu.VMEM((9, rows, cols), F32),
            pltpu.VMEM((12, rows, 128), F32),
            pltpu.VMEM((3, 128, 128), F32),
            pltpu.VMEM((3, 9, 40, 128), F32),
            pltpu.VMEM((4, 7, cols, 128), F32),
            pltpu.VMEM((rows, cols, nv), F32),
            pltpu.VMEM((2, 2, cols, nv), F32),
            pltpu.VMEM((4, rows, nv), F32),
            pltpu.VMEM((2, 2, rows, nv), F32),
            pltpu.VMEM((2, 8, nv), F32),
            pltpu.VMEM((2, 8, nv), F32),
            pltpu.VMEM((2, 2, rows, width), F32),
            pltpu.VMEM((6, 2, cols, width), F32),
            pltpu.VMEM((4, 4, NEAR * width), F32),
            pltpu.VMEM((4, 4, NEAR * width), F32),
            pltpu.VMEM((2, 8, 128), F32),
            pltpu.VMEM((2, 8, 128), F32),
            pltpu.VMEM((8, 8, 128), F32),
            dma, dma((2,)), pltpu.SemaphoreType.REGULAR, dma,
            dma, dma,
            dma((2,)), dma((CHUNKS,)),
            dma((2,)), dma((2, CHUNKS // GROUP)),
            dma((2,)), dma((CHUNKS - NEAR,)),
            dma((2,)), dma,
            dma((6,)), dma,
            dma, dma,
        ],
        compiler_params=pltpu.CompilerParams(collective_id=0, has_side_effects=True, vmem_limit_bytes=44 * 2**20),
    )(pltpu.with_memory_space_constraint(coefficients, pltpu.HBM), vectors)
    return pl.pallas_call(
        last_chunks,
        out_shape=(jax.ShapeDtypeStruct((25, rows, cols), F32), jax.ShapeDtypeStruct((rows, cols, nv), F32)),
        in_specs=[pl.BlockSpec(memory_space=pltpu.VMEM)] * 6,
        out_specs=(pl.BlockSpec(memory_space=pltpu.HBM),) * 2,
        scratch_shapes=[pltpu.VMEM((LAG, 4, 8, cols, width), F32), dma, dma],
        compiler_params=pltpu.CompilerParams(vmem_limit_bytes=8 * 2**20),
    )(*parts)


def solution(mesh):
    in_specs = (P(None, "gy", "gx"), P("gy", "gx", None))
    out_specs = (P(None, "gy", "gx"), P("gy", "gx", None))

    def whole(coefficients, vectors):
        body = functools.partial(per_device, coefficients.shape[1], coefficients.shape[2])
        return jax.shard_map(body, mesh=mesh, in_specs=in_specs, out_specs=out_specs, check_vma=False)(coefficients, vectors)

    return whole
```

```python
import functools

import jax
import jax.numpy as jnp
from jax import lax
from jax.experimental import pallas as pl
from jax.experimental.pallas import tpu as pltpu
from jax.sharding import PartitionSpec as P

MESH = pl.DeviceIdType.MESH
F32 = jnp.float32
BF16 = jnp.bfloat16
STEPS = ((-1, 0), (1, 0), (0, -1), (0, 1), (-1, -1), (-1, 1), (1, -1), (1, 1))
UP, DOWN, LEFT, RIGHT = 0, 1, 2, 3
CHUNKS = 8
GROUP = 4
LAG = 3
SETS = LAG + 1
NEAR = 3
SLOTS = [((m // 3 - k // 3) + 2) * 5 + (m % 3 - k % 3) + 2 for k in range(9) for m in range(9)]


RELAYS = (12, 11, 15), (3, 4, 0)
TURN = 7


def kernel(
    rows_total, cols_total,
    coef_hbm, v_hbm, normal_ref, image_ref, t_hi, t_lo, w_hi, w_lo,
    coef, padded, flipped, shifted, nts,
    v_vm, row_vm, col_vm, col_out, corner_out, corner_vm, relay_vm, hop_vm, diag_out, diag_vm,
    row_msg, col_msg, heard,
    load_sem, edge_sem, ready_sem, coef_sem, msg_send, msg_recv, row_send, row_recv, col_send, col_recv, cor_send, cor_recv,
    relay_recv, relay_send, hop_recv, hop_send, diag_send, diag_recv,
):
    gy = lax.axis_index("gy")
    gx = lax.axis_index("gx")
    ny = lax.axis_size("gy")
    nx = lax.axis_size("gx")
    rows, cols, nv = v_hbm.shape
    width = nv // CHUNKS

    def exists(n):
        dy, dx = STEPS[n]
        return (gy + dy >= 0) & (gy + dy < ny) & (gx + dx >= 0) & (gx + dx < nx)

    def at(n):
        dy, dx = STEPS[n]
        return (gy + dy, gx + dx)

    def lanes(i):
        return pl.ds(pl.multiple_of(i * width, width), width)

    up_vm, down_vm = row_vm.at[0], row_vm.at[1]

    def span(n):
        return pl.ds(0, n * width)

    def load(first, count, sem):
        part = pl.ds(first, count)
        return pltpu.make_async_copy(v_hbm.at[part], v_vm.at[part], sem)

    def row_copy(s, i):
        src = v_vm.at[0:2, :, lanes(i)] if s == UP else v_vm.at[rows - 2:rows, :, lanes(i)]
        dst = down_vm if s == UP else up_vm
        return pltpu.make_async_remote_copy(
            src_ref=src, dst_ref=dst.at[:, :, lanes(i)], send_sem=row_send.at[s],
            recv_sem=row_recv.at[i], device_id=at(s), device_id_type=MESH)

    odd = gy % 2 == 1
    plane = gy // 2
    crossing = (jnp.logical_not(odd), odd)
    late = jnp.where(odd, 2 * plane + 2, CHUNKS - 2 * plane)
    relaying = jnp.where(odd, gy >= 2, gy < ny - 2)
    held = jnp.where(odd, 2 * plane, jnp.maximum(CHUNKS - 2 - 2 * plane, 0))

    def hop(s, i, count):
        src = v_vm.at[0:2, :, lanes(i)] if s == UP else v_vm.at[rows - 2:rows, :, lanes(i)]
        slot = i - CHUNKS + count
        return pltpu.make_async_remote_copy(
            src_ref=src, dst_ref=hop_vm.at[slot], send_sem=row_send.at[s], recv_sem=hop_recv.at[slot],
            device_id=(gy + (2 if s == DOWN else -2), gx), device_id_type=MESH)

    def send_rows(i):
        for s in (UP, DOWN):
            detoured = crossing[s] & (i >= CHUNKS - late)
            when(exists(s) & jnp.logical_not(detoured), lambda s=s: row_copy(s, i).start())

    def send_hops(i):
        for s in (UP, DOWN):
            when(exists(s) & crossing[s] & (i >= CHUNKS - late), lambda s=s: hop(s, i, late).start())

    def hop_on(s, slot):
        i = CHUNKS - held + slot
        return pltpu.make_async_remote_copy(
            src_ref=hop_vm.at[slot], dst_ref=(down_vm if s == UP else up_vm).at[:, :, lanes(i)],
            send_sem=hop_send, recv_sem=row_recv.at[i],
            device_id=(gy + (1 if s == UP else -1), gx), device_id_type=MESH)

    def each_held(slots, f, only=True):
        for s in (UP, DOWN):
            for slot in slots:
                when(crossing[s] & (slot < held) & only, functools.partial(f, s, slot))

    def hop_pass(s, slot):
        hop(s, CHUNKS - held + slot, held).wait_recv()
        hop_on(s, slot).start()

    def col_copy(s, i):
        j = 2 - 2 * s
        return pltpu.make_async_remote_copy(
            src_ref=col_out.at[s, :, :, lanes(i)], dst_ref=col_vm.at[j:j + 2, 0:rows, lanes(i)],
            send_sem=col_send.at[s], recv_sem=col_recv.at[s, i // GROUP], device_id=at(LEFT + s), device_id_type=MESH)

    turns = ((gx == TURN + 1), (gx == TURN))

    def detour(s, i, n):
        slot = jnp.where(n == 2, i - 6, i // 3)
        first, second, third = RELAYS[1 - s]
        via = jnp.where(n == 2, third, jnp.where(n == 0, first, second))
        return pltpu.make_async_remote_copy(
            src_ref=col_out.at[s, :, :, lanes(i)], dst_ref=relay_vm.at[slot],
            send_sem=col_send.at[s], recv_sem=relay_recv.at[slot], device_id=(gy, via), device_id_type=MESH)

    def send_cols(s, i):
        around = turns[s] & ((i % 3 < 2) | (i >= 6))
        when(exists(LEFT + s) & jnp.logical_not(around), lambda: col_copy(s, i).start())
        when(around, lambda: detour(s, i, jnp.where(i >= 6, 2, i % 3)).start())

    def pass_on(slot, late):
        for s in (0, 1):
            for n, via in enumerate(RELAYS[1 - s]):
                if late == (n == 2):
                    i = 6 + slot if late else n + 3 * slot

                    def one(s=s, n=n, i=i):
                        detour(s, i, n).wait_recv()
                        j = 2 - 2 * s
                        pltpu.make_async_remote_copy(
                            src_ref=relay_vm.at[slot], dst_ref=col_vm.at[j:j + 2, 0:rows, lanes(i)], send_sem=relay_send,
                            recv_sem=col_recv.at[s, i // GROUP], device_id=(gy, TURN + s), device_id_type=MESH).start()

                    when(gx == via, one)

    def cor_copy(s, i):
        return pltpu.make_async_remote_copy(
            src_ref=corner_out.at[s, :, lanes(i)], dst_ref=corner_vm.at[s, :, lanes(i)],
            send_sem=cor_send.at[s], recv_sem=cor_recv.at[i], device_id=at(LEFT + s), device_id_type=MESH)

    def msg_copy(n):
        dy, dx = STEPS[n]
        src = row_msg.at[(dy + 1) // 2] if dy else col_msg.at[(dx + 1) // 2]
        return pltpu.make_async_remote_copy(
            src_ref=src, dst_ref=heard.at[n], send_sem=msg_send, recv_sem=msg_recv,
            device_id=at(n), device_id_type=MESH)

    def diag_copy(n):
        return pltpu.make_async_remote_copy(
            src_ref=diag_out.at[n - 4], dst_ref=diag_vm.at[n - 4], send_sem=diag_send,
            recv_sem=diag_recv, device_id=at(n), device_id_type=MESH)

    opposite = [STEPS.index((-dy, -dx)) for dy, dx in STEPS]

    def when(pred, f):
        pl.when(pred)(f)

    take_coef = pltpu.make_async_copy(coef_hbm, coef, coef_sem)
    barrier = pltpu.get_barrier_semaphore()
    take_coef.start()
    load(0, 2, edge_sem.at[0]).start()
    load(rows - 2, 2, edge_sem.at[1]).start()
    known = jnp.int32(0)
    for n in range(4):
        when(exists(n), lambda n=n: pl.semaphore_signal(barrier, inc=1, device_id=at(n), device_id_type=MESH))
        known = known + exists(n).astype(jnp.int32)
    for dy in (-2, 2):
        there = (gy + dy >= 0) & (gy + dy < ny)
        when(there, lambda dy=dy: pl.semaphore_signal(barrier, inc=1, device_id=(gy + dy, gx), device_id_type=MESH))
        known = known + there.astype(jnp.int32)
    for side in RELAYS:
        for via in side:
            for end in (TURN, TURN + 1):
                for me, other in ((via, end), (end, via)):
                    when(gx == me, lambda other=other: pl.semaphore_signal(barrier, inc=1, device_id=(gy, other), device_id_type=MESH))
                    known = known + (gx == me).astype(jnp.int32)
    padded[...] = jnp.zeros_like(padded)
    row_msg[...] = jnp.zeros_like(row_msg)
    col_msg[...] = jnp.zeros_like(col_msg)
    flipped[...] = jnp.zeros_like(flipped)
    take_coef.wait()
    load(2, rows - 4, load_sem).start()
    padded[0:9, :, 0:cols] = coef[...]
    lane = lax.broadcasted_iota(jnp.int32, (8, 128), 1)
    for e, r in ((0, 0), (1, rows - 1)):
        for k in range(8):
            row_msg[e, k:k + 1, :] = padded[k, r:r + 1, :]
        last = pltpu.roll(jnp.broadcast_to(padded[8, r:r + 1, :], (8, 128)), 32, 1)
        row_msg[e] = jnp.where((lane >= 32) & (lane < 64), last, row_msg[e])
    for g in range(3):
        turned = padded[4 * g:4 * g + 4].reshape(128, 128).T
        col_msg[0, g:g + 1, :] = turned[0:1]
        col_msg[1, g:g + 1, :] = turned[cols - 1:cols]
        flipped[g, 1:cols + 1, :] = turned[0:cols]
    load(0, 2, edge_sem.at[0]).wait()
    load(rows - 2, 2, edge_sem.at[1]).wait()
    pl.semaphore_wait(barrier, known)

    for n in (LEFT, RIGHT):
        when(exists(n), lambda n=n: pl.semaphore_signal(ready_sem, inc=1, device_id=at(n), device_id_type=MESH))
    for n in range(4):
        when(exists(n), lambda n=n: msg_copy(n).start())
    send_rows(0)
    pl.semaphore_wait(ready_sem, exists(LEFT).astype(jnp.int32) + exists(RIGHT).astype(jnp.int32))
    for n in range(4, 8):
        when(exists(n), lambda n=n: msg_copy(n).start())

    def rest(i, c):
        send_rows(i)
        return c

    def hops(i, c):
        send_hops(i)
        return c

    lax.fori_loop(2, CHUNKS, hops, 0)

    lax.fori_loop(1, CHUNKS - 3, rest, 0)

    def clear(ref):
        ref[...] = jnp.zeros_like(ref)

    when(jnp.logical_not(exists(UP)), lambda: clear(up_vm))
    when(jnp.logical_not(exists(DOWN)), lambda: clear(down_vm))
    for s in (0, 1):
        j = 2 - 2 * s
        when(jnp.logical_not(exists(LEFT + 1 - s)), lambda s=s, j=j: (clear(col_vm.at[j:j + 2]), clear(corner_vm.at[s]))[0])

    def pack(i, c):
        for s in (0, 1):
            for j in (0, 1):
                col = j if s == 0 else cols - 2 + j
                for r in range(0, rows, 8):
                    col_out[s, j, r:r + 8, lanes(i)] = v_vm[r:r + 8, col, lanes(i)]
        for s in (0, 1):
            send_cols(s, i)
        return c

    load(2, rows - 4, load_sem).wait()
    lax.fori_loop(0, CHUNKS, pack, 0)
    for n in range(4, 8):
        dy, dx = STEPS[n]
        for c in (0, 1):
            for h in (0, 1):
                row, col = (h if dy < 0 else rows - 2 + h), (c if dx < 0 else cols - 2 + c)
                diag_out[n - 4, 2 * c + h:2 * c + h + 1, :] = v_vm[row, col:col + 1, nv - NEAR * width:nv]
        when(exists(n), lambda n=n: diag_copy(n).start())
        when(jnp.logical_not(exists(opposite[n])), lambda n=n: clear(diag_vm.at[n - 4]))

    def sent(ref, sem):
        pltpu.make_async_copy(ref, ref, sem).wait()

    neighbours = jnp.int32(0)
    for n in range(8):
        neighbours = neighbours + exists(n).astype(jnp.int32)

    def messages(sem):
        for n in (3, 5, 8):
            when(neighbours == n, lambda n=n: sent(heard.at[0:n], sem))

    corners = jnp.int32(0)
    for n in range(4, 8):
        corners = corners + exists(n).astype(jnp.int32)

    def diagonals(sem):
        for n in (1, 2, 4):
            when(corners == n, lambda n=n: sent(diag_vm.at[0:n], sem))

    def both_or_one(a, b, both, one, sem, i):
        pair = exists(a) & exists(b)
        when(pair, lambda: sent(both, sem.at[i]))
        when(jnp.logical_not(pair), lambda: sent(one, sem.at[i]))

    messages(msg_recv)

    def from_side(n):
        return heard[opposite[n]]

    for g in range(3):
        flipped[g, 0:1, :] = jnp.where(exists(LEFT), from_side(LEFT)[g:g + 1], 0.0)
        flipped[g, cols + 1:cols + 2, :] = jnp.where(exists(RIGHT), from_side(RIGHT)[g:g + 1], 0.0)

    def rim(side, left, right):
        out = []
        for own, a, b in ((1, 97, 33), (97, 65, 1)):
            x = jnp.where(exists(side), pltpu.roll(from_side(side), own, 1), 0.0)
            x = jnp.where((lane == 0), jnp.where(exists(left), pltpu.roll(from_side(left), a, 1), 0.0), x)
            x = jnp.where((lane == cols + 1), jnp.where(exists(right), pltpu.roll(from_side(right), b, 1), 0.0), x)
            out.append(x)
        return out

    above = rim(UP, 4, 5)
    below = rim(DOWN, 6, 7)
    er = lax.broadcasted_iota(jnp.int32, (40, 128), 0)
    ec = lax.broadcasted_iota(jnp.int32, (40, 128), 1)
    row_at = gy * rows + er - 1
    col_at = gx * cols + ec - 1
    inside = (er < rows + 2) & (ec < cols + 2) & (row_at >= 0) & (row_at < rows_total) & (col_at >= 0) & (col_at < cols_total)
    for g in range(3):
        back = flipped[g].T
        for h in range(4):
            k = 4 * g + h
            if k < 9:
                a, b = k // 3 - 1, k % 3 - 1
                shifted[0, k, 1:rows + 1, :] = back[32 * h:32 * h + rows]
                which, line = (0, k) if k < 8 else (1, 0)
                shifted[0, k, 0:1, :] = above[which][line:line + 1]
                shifted[0, k, rows + 1:rows + 2, :] = below[which][line:line + 1]
                keep = inside & (row_at + a >= 0) & (row_at + a < rows_total) & (col_at + b >= 0) & (col_at + b < cols_total)
                x = jnp.where(keep, shifted[0, k], 0.0)
                shifted[0, k] = x
                shifted[1, k] = pltpu.roll(x, 127, 1)
                shifted[2, k] = pltpu.roll(x, 126, 1)
    terms = []
    for slot in range(25):
        total = None
        for at_pair in range(81):
            if SLOTS[at_pair] == slot:
                k, m = at_pair // 9, at_pair % 9
                a, b = k // 3 - 1, k % 3 - 1
                term = shifted[1 - b, k, 1 - a:1 - a + rows, :] * shifted[1 - b, m, 1 - a:1 - a + rows, :]
                total = term if total is None else total + term
        normal_ref[slot] = total[:, 0:cols]
        terms.append(total)
    for g in range(7):
        group = terms[4 * g:4 * g + 4]
        while len(group) < 4:
            group.append(jnp.zeros_like(group[0]))
        turned = jnp.concatenate(group, axis=0).T[0:cols]
        nts[0, g] = turned
        for b in range(1, 4):
            nts[b, g] = pltpu.roll(turned, 128 - 8 * b, 1)

    lane32 = lax.broadcasted_iota(jnp.int32, (cols, 128), 1)
    cell = lax.broadcasted_iota(jnp.int32, (cols, 128), 0)
    own_at, side_at = {}, {}
    for f in range(-2, 3):
        t = cell + f
        own_at[f] = jnp.where((t >= 0) & (t < cols), t, -1000)
        side_at[f] = jnp.where(t == -2, 0, jnp.where(t == -1, 32, jnp.where(t == cols, 64, jnp.where(t == cols + 1, 96, -1000))))

    def build(b, c):
        for rl in range(8):
            own = [jnp.zeros((cols, 128), F32) for _ in range(3)]
            side = jnp.zeros((cols, 128), F32)
            for e in range(-2, 3):
                spot = rl + e + 2
                tile, q = spot // 4, spot % 4
                row = b * 8 + rl + e
                slot = jnp.where(row < 0, 18 + row, row)
                slot = jnp.where(b == 3, jnp.where(row < rows, row - 16, row - 14), slot)
                for f in range(-2, 3):
                    index = (e + 2) * 5 + f + 2
                    at_lane = (index % 4) * 32 + rl
                    column = jnp.broadcast_to(nts[b, index // 4][:, at_lane:at_lane + 1], (cols, 128))
                    own[tile] = jnp.where(lane32 - 32 * q == own_at[f], column, own[tile])
                    if f:
                        side = jnp.where(lane32 - slot == side_at[f], column, side)
            for tile, x in enumerate(own + [side]):
                hi = x.astype(BF16)
                t_hi[b, rl * 32:rl * 32 + 32, tile * 128:tile * 128 + 128] = hi
                t_lo[b, rl * 32:rl * 32 + 32, tile * 128:tile * 128 + 128] = (x - hi.astype(F32)).astype(BF16)
        return c

    each_held((0, 1), hop_pass, held > 2)
    send_rows(CHUNKS - 3)
    lax.fori_loop(0, 2, build, 0)
    pass_on(0, False)
    each_held((2,), hop_pass)
    send_rows(CHUNKS - 2)
    lax.fori_loop(2, 4, build, 0)
    pass_on(1, False)
    each_held((3,), hop_pass)
    each_held((0, 1), hop_pass, held == 2)
    send_rows(CHUNKS - 1)

    def halves(x):
        hi = x.astype(BF16)
        return hi, (x - hi.astype(F32)).astype(BF16)

    def put(i, block, start, hi, lo):
        w_hi[i % SETS, block, start:start + hi.shape[0], :] = hi
        w_lo[i % SETS, block, start:start + hi.shape[0], :] = lo

    def own_part(i):
        for q in range(4):
            hi, lo = halves(v_vm[8 * q:8 * q + 8, :, lanes(i)].reshape(256, width))
            put(i, q, 64, hi, lo)
            if q > 0:
                put(i, q - 1, 320, hi[0:64], lo[0:64])
            if q < 3:
                put(i, q + 1, 0, hi[192:256], lo[192:256])

    def side_part(i, near=None):
        def columns(s):
            j = 2 - 2 * s
            at_group = pl.ds(pl.multiple_of(i * width, width), GROUP * width)
            whole = col_vm.at[j:j + 2, 0:rows, at_group]
            pltpu.make_async_copy(whole, whole, col_recv.at[s, i // GROUP]).wait()

        if near is None:
            for s in (0, 1):
                when(exists(LEFT + 1 - s) & (i % GROUP == 0), functools.partial(columns, s))
            both_or_one(LEFT, RIGHT, corner_vm.at[:, :, lanes(i)], corner_vm.at[0, :, lanes(i)], cor_recv, i)
        for j in range(4):
            hi, lo = halves(col_vm[j, 0:32, lanes(i)])
            if near is not None:
                at_near = slice(near * width, near * width + width)
                from_above, from_below = (6, 4) if j >= 2 else (7, 5)
                c = 2 * (j % 2)
                corner = jnp.concatenate([
                    diag_vm[from_above - 4, c:c + 2, at_near], diag_vm[from_below - 4, c:c + 2, at_near], jnp.zeros((12, width), F32)], axis=0)
            else:
                c = 4 * (j % 2)
                corner = jnp.concatenate([corner_vm[1 - j // 2, c:c + 4, lanes(i)], jnp.zeros((12, width), F32)], axis=0)
            chi, clo = halves(corner)
            put(i, 0, 384 + 32 * j, hi[0:16], lo[0:16])
            put(i, 0, 400 + 32 * j, chi, clo)
            put(i, 1, 384 + 32 * j, hi, lo)
            put(i, 2, 384 + 32 * j, hi, lo)
            put(i, 3, 384 + 32 * j, hi[16:32], lo[16:32])
            put(i, 3, 400 + 32 * j, chi, clo)

    def compute(i):
        side_part(i)
        for q in range(4):
            y = products(t_hi[q], t_lo[q], w_hi[i % SETS, q], w_lo[i % SETS, q])
            image_ref[8 * q:8 * q + 8, :, lanes(i)] = y.reshape(8, cols, width)

    turned = turns[0] | turns[1]

    def computed(i):
        late_count = jnp.clip(i - 2, 0, CHUNKS - LAG)
        return jnp.where(turned | (i < CHUNKS - 3), late_count, jnp.minimum(i - 1, CHUNKS - LAG))

    def main(i, c):
        for step, slots in ((1, (4,)), (2, (5,))):
            when(i == step, lambda slots=slots: each_held(slots, hop_pass))
        for step in (3, 4):
            when(i == step, functools.partial(pass_on, step - 3, True))
        own_part(i)
        lax.fori_loop(computed(i - 1), computed(i), lambda c, x: (compute(c), x)[1], 0)
        both_or_one(UP, DOWN, row_vm.at[:, :, :, lanes(i)], up_vm.at[:, :, lanes(i)], row_recv, i)
        for s in (0, 1):
            for j in (0, 1):
                col = j if s == 0 else cols - 2 + j
                for h in (0, 1):
                    corner_out[s, 4 * j + h:4 * j + h + 1, lanes(i)] = up_vm[h, col:col + 1, lanes(i)]
                    corner_out[s, 4 * j + 2 + h:4 * j + 3 + h, lanes(i)] = down_vm[h, col:col + 1, lanes(i)]
            when(exists(LEFT + s) & (i < CHUNKS - NEAR), lambda s=s: cor_copy(s, i).start())
        put(i, 0, 0, *halves(up_vm[:, :, lanes(i)].reshape(64, width)))
        put(i, 3, 320, *halves(down_vm[:, :, lanes(i)].reshape(64, width)))
        return c

    lax.fori_loop(0, CHUNKS, main, 0)
    for i in range(CHUNKS - LAG, CHUNKS - NEAR):
        side_part(i)
    diagonals(diag_recv)
    for near in range(NEAR):
        side_part(CHUNKS - NEAR + near, near)

    for s in (0, 1):
        when(exists(s), lambda s=s: sent(up_vm, row_send.at[s]))
        when(exists(LEFT + s), lambda s=s: sent(col_out.at[s], col_send.at[s]))
        when(exists(LEFT + s), lambda s=s: sent(corner_out.at[s, :, span(CHUNKS - NEAR)], cor_send.at[s]))
    diagonals(diag_send)
    messages(msg_send)
    for side in RELAYS:
        for via in side:
            when(gx == via, lambda: sent(relay_vm, relay_send))
    for n in (2, 4, 6):
        when(relaying & (held == n), lambda n=n: sent(hop_vm.at[0:n], hop_send))


def products(t_hi, t_lo, w_hi, w_lo):
    y = jnp.dot(t_hi, w_hi, preferred_element_type=F32)
    y = y + jnp.dot(t_lo, w_hi, preferred_element_type=F32)
    return y + jnp.dot(t_hi, w_lo, preferred_element_type=F32)


def last_chunks(normal_vm, image_vm, t_hi, t_lo, w_hi, w_lo, normal_hbm, image_hbm, tail, normal_sem, image_sem):
    rows, cols, nv = image_hbm.shape
    width = nv // CHUNKS
    done = nv - LAG * width
    for q in range(4):
        pltpu.make_async_copy(
            image_vm.at[8 * q:8 * q + 8, :, :], image_hbm.at[8 * q:8 * q + 8, :, 0:done], image_sem).start()
    write_normal = pltpu.make_async_copy(normal_vm, normal_hbm, normal_sem)
    write_normal.start()
    for n in range(LAG):
        i = CHUNKS - LAG + n
        for q in range(4):
            y = products(t_hi[q], t_lo[q], w_hi[i % SETS, q], w_lo[i % SETS, q])
            tail[n, q] = y.reshape(8, cols, width)
            pltpu.make_async_copy(
                tail.at[n, q], image_hbm.at[8 * q:8 * q + 8, :, i * width:i * width + width], image_sem).start()
    pltpu.make_async_copy(image_hbm, image_hbm, image_sem).wait()
    write_normal.wait()


def per_device(rows_total, cols_total, coefficients, vectors):
    _, rows, cols = coefficients.shape
    nv = vectors.shape[2]
    width = nv // CHUNKS
    dma = pltpu.SemaphoreType.DMA
    parts = pl.pallas_call(
        functools.partial(kernel, rows_total, cols_total),
        out_shape=(
            pltpu.VMEM((25, rows, cols), F32), pltpu.VMEM((rows, cols, nv - LAG * width), F32),
            pltpu.VMEM((4, 256, 512), BF16), pltpu.VMEM((4, 256, 512), BF16),
            pltpu.VMEM((SETS, 4, 512, width), BF16), pltpu.VMEM((SETS, 4, 512, width), BF16)),
        in_specs=[pl.BlockSpec(memory_space=pltpu.HBM)] * 2,
        out_specs=(pl.BlockSpec(memory_space=pltpu.VMEM),) * 6,
        scratch_shapes=[
            pltpu.VMEM((9, rows, cols), F32),
            pltpu.VMEM((12, rows, 128), F32),
            pltpu.VMEM((3, 128, 128), F32),
            pltpu.VMEM((3, 9, 40, 128), F32),
            pltpu.VMEM((4, 7, cols, 128), F32),
            pltpu.VMEM((rows, cols, nv), F32),
            pltpu.VMEM((2, 2, cols, nv), F32),
            pltpu.VMEM((4, rows, nv), F32),
            pltpu.VMEM((2, 2, rows, nv), F32),
            pltpu.VMEM((2, 8, nv), F32),
            pltpu.VMEM((2, 8, nv), F32),
            pltpu.VMEM((2, 2, rows, width), F32),
            pltpu.VMEM((6, 2, cols, width), F32),
            pltpu.VMEM((4, 4, NEAR * width), F32),
            pltpu.VMEM((4, 4, NEAR * width), F32),
            pltpu.VMEM((2, 8, 128), F32),
            pltpu.VMEM((2, 8, 128), F32),
            pltpu.VMEM((8, 8, 128), F32),
            dma, dma((2,)), pltpu.SemaphoreType.REGULAR, dma,
            dma, dma,
            dma((2,)), dma((CHUNKS,)),
            dma((2,)), dma((2, CHUNKS // GROUP)),
            dma((2,)), dma((CHUNKS - NEAR,)),
            dma((2,)), dma,
            dma((6,)), dma,
            dma, dma,
        ],
        compiler_params=pltpu.CompilerParams(collective_id=0, has_side_effects=True, vmem_limit_bytes=44 * 2**20),
    )(pltpu.with_memory_space_constraint(coefficients, pltpu.HBM), vectors)
    return pl.pallas_call(
        last_chunks,
        out_shape=(jax.ShapeDtypeStruct((25, rows, cols), F32), jax.ShapeDtypeStruct((rows, cols, nv), F32)),
        in_specs=[pl.BlockSpec(memory_space=pltpu.VMEM)] * 6,
        out_specs=(pl.BlockSpec(memory_space=pltpu.HBM),) * 2,
        scratch_shapes=[pltpu.VMEM((LAG, 4, 8, cols, width), F32), dma, dma],
        compiler_params=pltpu.CompilerParams(vmem_limit_bytes=8 * 2**20),
    )(*parts)


def solution(mesh):
    in_specs = (P(None, "gy", "gx"), P("gy", "gx", None))
    out_specs = (P(None, "gy", "gx"), P("gy", "gx", None))

    def whole(coefficients, vectors):
        body = functools.partial(per_device, coefficients.shape[1], coefficients.shape[2])
        return jax.shard_map(body, mesh=mesh, in_specs=in_specs, out_specs=out_specs, check_vma=False)(coefficients, vectors)

    return whole
```
